128 devices in a mesh: facet: 16 (over y, x), chan: 8 (over z, core).
Axes of the slice: x: 4, y: 4, z: 4, core: 2. Of those that a mesh axis runs over, the one named last changes fastest.
Arguments:
- model_taylor: float32 [2, 16, 2, 512, 512], P(None, 'facet'), may hold values from -6 to 6
- channel_offset: float32 [8], P('chan'), may hold values from -0.5 to 0.5
- assignment: int32 [16], replicated, may hold values from 0 to 15, each once
- observed: float32 [8, 16, 2, 4096], P('chan', 'facet'), may hold values from -12 to 12
- uv_bins: int32 [8, 16, 4096], P('chan', 'facet'), may hold values from 0 to 16383
- vis_counts: int32 [8, 16], P('chan', 'facet'), may hold values from 1 to 4096, 32768 in all within a row
Outputs:
- taylor_residual: float32 [2, 16, 2, 512, 512], P(None, 'facet', None, 'chan')
The draws below stay inside these ranges and needn't reach their ends.
Inputs may be any that keep to these rules, and one draw needn't show every extreme that they name: A permutation: task t, held by helper t, works on subgrid assignment[t]. Slots 0 .. vis_counts - 1 of a task are live; the others are ignored.
All inputs are finite; a program needn't handle non-finite values. No bound on the sum of `vis_counts` on one device may be relied on, other than what follows from the above.
Results may differ from the reference program's by a relative error of at most 0.0003.
Values sent between devices are 32-bit elements; how exact they have to be, the bound alone decides.
No kernel may reach another device: no remote copies, remote signals or barrier semaphores. Data moves between devices by JAX's collectives and lax.ppermute only.
A program may use at most 128 MiB of HBM per device.

```python
import math
import jax
import jax.numpy as jnp
import numpy as np
from jax import lax

FS = 512
XM = 128
FACET_COLS = 4
SUB_COLS = 4
VIS = 4096
NF = 16
NSUB = 16
CHANS = 8
IMAGE = 2048


def set_ends(entries, rng, smallest, top_value):
    longest = entries.shape.index(max(entries.shape))
    spots = []
    for shift in (0, 1):
        where = [jax.random.randint(jax.random.fold_in(rng, axis), (), 0, length) for axis, length in enumerate(entries.shape)]
        where[longest] = (where[longest] + shift) % entries.shape[longest]
        spots.append(tuple(where))
    return entries.at[spots[0]].set(smallest).at[spots[1]].set(top_value)


def block_scale(key, dims, shards, smallest, largest):
    gain = 1.0
    for position, blocks in shards:
        heights = jax.random.uniform(jax.random.fold_in(jax.random.fold_in(key, 6), position), (blocks,), jnp.float32, smallest / len(shards), largest / len(shards))
        gain = gain * jnp.repeat(jnp.exp(heights), dims[position] // blocks).reshape((-1,) + (1,) * (len(dims) - 1 - position))
    return gain


def length_profile(number_of, total, limit, lean):
    weights = [(1 << 20) // math.isqrt(rank ** lean) + 1 for rank in range(2, number_of + 1)]
    surplus, given = total - limit - (number_of - 1), [1] * (number_of - 1)
    while surplus > 0:
        candidates = [i for i in range(number_of - 1) if given[i] < limit]
        mass, budget = sum([weights[i] for i in candidates]), surplus
        for i in candidates:
            more = min(limit - given[i], max(1, budget * weights[i] // mass), surplus)
            given[i] = given[i] + more
            surplus = surplus - more
    return np.array([limit] + given)


def uneven_parts(stream_key, count, total, reach, lean):
    if count == 2:
        one = jax.random.randint(stream_key, (), max(1, total - reach), min(reach, total - 1) + 1)
        return jnp.stack([one, total - one])
    sizes = jnp.asarray(length_profile(count, total, reach, lean), jnp.int32)
    pairs = (count - 1) // 2
    donor, receiver = sizes[1:1 + 2 * pairs:2], sizes[2:2 + 2 * pairs:2]
    room = jnp.minimum(donor - 1, reach - receiver)
    shifted = jax.random.randint(jax.random.fold_in(stream_key, 1), (pairs,), 0, 1 << 20) % (room + 1)
    sizes = sizes.at[1:1 + 2 * pairs:2].set(donor - shifted).at[2:2 + 2 * pairs:2].set(receiver + shifted)
    return sizes[jax.random.permutation(jax.random.fold_in(stream_key, 2), count)]


def gaussian(rng, shape, scale, limit, pieces=(), kind=jnp.bfloat16):
    entries = scale * jax.random.normal(rng, shape, jnp.float32)
    if pieces:
        entries = entries * block_scale(rng, shape, pieces, -0.22, 0.18)
    return jnp.clip(entries, -limit, limit).astype(kind)


def setup_inputs(seed: int = 0) -> dict:
    seeds = jax.random.split(jax.random.key(seed), 7)
    model_taylor = gaussian(seeds[0], (2, NF, 2, FS, FS), 1.0, 6.0, ((1, 16),), jnp.float32)
    channel_offset = jnp.clip(jax.random.uniform(seeds[1], (CHANS,), jnp.float32, -0.5, 0.5) * block_scale(seeds[1], (CHANS,), ((0, 8),), -0.4, 0.0), -0.5, 0.5)
    assignment = jax.random.permutation(seeds[2], NSUB).astype(jnp.int32)
    observed = gaussian(seeds[3], (CHANS, NSUB, 2, VIS), 2.0, 12.0, ((0, 8), (1, 16)), jnp.float32)
    uv_bins = set_ends(jax.random.randint(seeds[4], (CHANS, NSUB, VIS), 0, XM * XM), jax.random.fold_in(seeds[4], 1), 0, (XM * XM) - 1).astype(jnp.int32)
    vis_counts = jax.vmap(lambda own: uneven_parts(own, NSUB, NSUB * VIS // 2, VIS, 2))(jax.random.split(seeds[5], CHANS)).reshape((CHANS, NSUB)).astype(jnp.int32)
    return {"model_taylor": model_taylor, "channel_offset": channel_offset, "assignment": assignment, "observed": observed, "uv_bins": uv_bins, "vis_counts": vis_counts}


TWO_PI = 6.283185307179586
HIGHEST = lax.Precision.HIGHEST

def taper_values(length):
    positions = jnp.arange(length, dtype=jnp.float32)
    shaped = 0.55 + 0.45 * jnp.cos(jnp.pi * (2.0 * positions + 1.0 - length) / length)
    return shaped / jnp.sqrt(jnp.float32(length))

def phase_pair(frequency, pixels):
    product = frequency[:, None] * pixels[None, :] % IMAGE
    angle = product.astype(jnp.float32) * (TWO_PI / IMAGE)
    return (jnp.cos(angle), -jnp.sin(angle))

def row_table(facet_row, row_total):
    frequency = jnp.arange(row_total * XM, dtype=jnp.int32)
    pixels = facet_row * FS + jnp.arange(FS, dtype=jnp.int32)
    real_part, imag_part = phase_pair(frequency, pixels)
    window = taper_values(FS)[None, :]
    return jnp.concatenate([real_part * window, imag_part * window], axis=1)

def column_table(facet_col):
    frequency = jnp.arange(SUB_COLS * XM, dtype=jnp.int32)
    pixels = facet_col * FS + jnp.arange(FS, dtype=jnp.int32)
    real_part, imag_part = phase_pair(frequency, pixels)
    window = taper_values(FS)[None, :]
    real_part = (real_part * window).reshape(SUB_COLS, XM, FS).transpose(2, 0, 1)
    imag_part = (imag_part * window).reshape(SUB_COLS, XM, FS).transpose(2, 0, 1)
    upper_rows = jnp.stack([real_part, imag_part], axis=2).reshape(FS, SUB_COLS * 2 * XM)
    lower_rows = jnp.stack([-imag_part, real_part], axis=2).reshape(FS, SUB_COLS * 2 * XM)
    return jnp.concatenate([upper_rows, lower_rows], axis=0)

def predict(sky_image, rows_tab, cols_fwd, row_total):
    joined = jnp.concatenate([sky_image[0], sky_image[1]], axis=1)
    prepared = jnp.dot(joined, cols_fwd, precision=HIGHEST, preferred_element_type=jnp.float32)
    prepared = prepared.reshape(FS, SUB_COLS, 2, XM)
    real_part = prepared[:, :, 0]
    imag_part = prepared[:, :, 1]
    upper_rows = jnp.stack([real_part, imag_part], axis=2).reshape(FS, SUB_COLS * 2 * XM)
    lower_rows = jnp.stack([-imag_part, real_part], axis=2).reshape(FS, SUB_COLS * 2 * XM)
    mixer = jnp.concatenate([upper_rows, lower_rows], axis=0)
    result = jnp.dot(rows_tab, mixer, precision=HIGHEST, preferred_element_type=jnp.float32)
    result = result.reshape(row_total, XM, SUB_COLS, 2, XM).transpose(0, 2, 3, 1, 4)
    return result.reshape(row_total * SUB_COLS, 2, XM, XM)

def adjoint_rows(rows_tab, row_total):
    return rows_tab.reshape(row_total * XM, 2, FS).transpose(1, 0, 2).reshape(2 * row_total * XM, FS)

def adjoint(uv_grids, rows_adj, cols_adj, row_total):
    arranged = uv_grids.reshape(row_total, SUB_COLS, 2, XM, XM).transpose(0, 3, 1, 2, 4)
    upper_rows = arranged.reshape(row_total * XM, SUB_COLS * 2 * XM)
    lower_rows = jnp.stack([arranged[:, :, :, 1], -arranged[:, :, :, 0]], axis=3)
    lower_rows = lower_rows.reshape(row_total * XM, SUB_COLS * 2 * XM)
    mixer = jnp.concatenate([upper_rows, lower_rows], axis=0)
    weighted = lax.dot_general(rows_adj, mixer, (((0,), (0,)), ((), ())), precision=HIGHEST, preferred_element_type=jnp.float32)
    joined = jnp.dot(weighted, cols_adj, precision=HIGHEST, preferred_element_type=jnp.float32)
    return joined.reshape(joined.shape[0], 2, FS).transpose(1, 0, 2)

def residual_grid(uv_grid, observed_one, cell_index, live_total):
    flat_grid = uv_grid.reshape(2, XM * XM)
    predicted = jnp.take(flat_grid, cell_index, axis=1)
    is_live = jnp.arange(cell_index.shape[0], dtype=jnp.int32) < live_total
    misfit = jnp.where(is_live[None, :], observed_one - predicted, 0.0)
    return jnp.zeros_like(flat_grid).at[:, cell_index].add(misfit).reshape(2, XM, XM)

def reference(model_taylor, channel_offset, assignment, observed, uv_bins, vis_counts):
    row_total = NSUB // SUB_COLS
    facet_ids = jnp.arange(NF, dtype=jnp.int32)

    def forward(running, facet_index):
        rows_tab = row_table(facet_index // FACET_COLS, row_total)
        cols_fwd = column_table(facet_index % FACET_COLS)
        terms = lax.dynamic_index_in_dim(model_taylor, facet_index, 1, keepdims=False)
        parts = jnp.stack([predict(terms[0], rows_tab, cols_fwd, row_total), predict(terms[1], rows_tab, cols_fwd, row_total)])
        return (running + parts, None)
    summed, _ = lax.scan(forward, jnp.zeros((2, NSUB, 2, XM, XM), jnp.float32), facet_ids)
    uv_grids = summed[0][None] + channel_offset[:, None, None, None, None] * summed[1][None]
    by_task = jnp.take(uv_grids, assignment, axis=1)
    misfits = jax.vmap(jax.vmap(residual_grid))(by_task, observed, uv_bins, vis_counts)
    ordered = jnp.zeros_like(misfits).at[:, assignment].set(misfits)
    weights = jnp.stack([jnp.ones_like(channel_offset), channel_offset])
    taylor = jnp.einsum('tc,csabk->tsabk', weights, ordered, precision=HIGHEST)

    def backward(facet_index):
        rows_adj = adjoint_rows(row_table(facet_index // FACET_COLS, row_total), row_total)
        cols_adj = column_table(facet_index % FACET_COLS).T
        return jnp.stack([adjoint(taylor[0], rows_adj, cols_adj, row_total), adjoint(taylor[1], rows_adj, cols_adj, row_total)])
    result = lax.map(backward, facet_ids)
    return jnp.transpose(result, (1, 0, 2, 3, 4))
```

```python
import jax
import jax.numpy as jnp
from jax import lax
from jax.experimental import pallas as pl
from jax.experimental.pallas import tpu as pltpu
from jax.sharding import PartitionSpec as P

FS = 512
XM = 128
SIDE = 4
NF = 16
CHANS = 8
VIS = 4096
IMAGE = 2048
PART = XM // CHANS
PIECE = 4 * PART
ROWS = VIS // XM
META = 3 * ROWS
MSG = META + 8
TILE = 8 * XM
TILES = VIS // TILE

TURN = 6.283185307179586 / IMAGE
F32 = jnp.float32
BF16 = jnp.bfloat16
VMEM = pl.BlockSpec(memory_space=pltpu.VMEM)
SMEM = pl.BlockSpec(memory_space=pltpu.SMEM)


def cos_turn(m):
    m = m & (IMAGE - 1)
    quarter = (m + 256) >> 9
    t = (m - (quarter << 9)).astype(F32) * TURN
    t2 = t * t
    even = 1.0 + t2 * (-0.5 + t2 * (1 / 24 + t2 * (-1 / 720 + t2 * (1 / 40320 - t2 * (1 / 3628800)))))
    odd = t * (1.0 + t2 * (-1 / 6 + t2 * (1 / 120 + t2 * (-1 / 5040 + t2 * (1 / 362880)))))
    value = jnp.where((quarter & 1) == 1, odd, even)
    return jnp.where(((quarter + 1) & 2) == 2, -value, value)


def taper(n):
    return (0.55 + 0.45 * cos_turn(4 * n - (2 * FS - 2))) * F32(1.0 / FS**0.5)


def halves(value):
    high = value.astype(BF16)
    return high, (value - high.astype(F32)).astype(BF16)


def iota(shape, dim):
    return lax.broadcasted_iota(jnp.int32, shape, dim)


def mm(a, b, dims=((1,), (0,))):
    return lax.dot_general(a, b, (dims, ((), ())), preferred_element_type=F32)


def mm3(a_high, a_low, b_high, b_low, dims=((1,), (0,))):
    return mm(a_high, b_high, dims) + (mm(a_high, b_low, dims) + mm(a_low, b_high, dims))


def position():
    facet = lax.axis_index("facet")
    return facet // SIDE, facet % SIDE, lax.axis_index("chan")


def quarter_turn(facet_row, facet_col):
    shape = (PART, XM)
    turn = (iota(shape, 1) * facet_row + iota(shape, 0) * facet_col) & 3
    real = jnp.where(turn == 0, 1.0, jnp.where(turn == 2, -1.0, 0.0)).astype(F32)
    imag = jnp.where(turn == 3, 1.0, jnp.where(turn == 1, -1.0, 0.0)).astype(F32)
    return real, imag


def pack_kernel(offset, count, observed, bins, out):
    live = iota((1, VIS), 1) < count[0, 0]
    cells = jnp.where(live, bins[...].astype(F32), -1.0)
    for row in range(ROWS):
        lanes = slice(row * XM, (row + 1) * XM)
        for dest in range(CHANS):
            out[dest, row : row + 1, :] = observed[0:1, lanes]
            out[dest, ROWS + row : ROWS + row + 1, :] = observed[1:2, lanes]
            out[dest, 2 * ROWS + row : 2 * ROWS + row + 1, :] = cells[:, lanes]
    place = iota((8, XM), 0)
    meta = jnp.where(place == 0, offset[0], jnp.where(place == 1, count[0, 0].astype(F32), 0.0))
    for dest in range(CHANS):
        out[dest, META:MSG, :] = meta


def forward_kernel(assignment, sky, table_high, table_low, out, cols_high, cols_low, rows, pieces):
    step = pl.program_id(0)
    facet_row, facet_col, part = position()

    @pl.when(step == 0)
    def tables():
        pixel = iota((PART, FS), 1)
        fine = iota((PART, FS), 0) * pixel
        fine_re, fine_im = cos_turn(fine), cos_turn(fine + 512)
        coarse = iota((FS // PART, FS), 0) * PART * iota((FS // PART, FS), 1)
        coarse_re, coarse_im = cos_turn(coarse), cos_turn(coarse + 512)
        for g in range(FS // PART):
            re, im = coarse_re[g : g + 1], coarse_im[g : g + 1]
            here = slice(g * PART, (g + 1) * PART)
            table_high[0, here], table_low[0, here] = halves(re * fine_re - im * fine_im)
            table_high[1, here], table_low[1, here] = halves(re * fine_im + im * fine_re)
        shape = (FS, 2 * SIDE * PART)
        y, lane = iota(shape, 0), iota(shape, 1)
        column = ((lane & 63) >> 4) * XM + part * PART + (lane & (PART - 1))
        turn = column * y + jnp.where(lane >= 64, 512, 0)
        window = taper(y)
        cols_high[0], cols_low[0] = halves(cos_turn(turn) * window)
        cols_high[1], cols_low[1] = halves(cos_turn(turn - 512) * window)

    plane = step & 1
    high, low = halves(sky[0, 0])
    made = mm3(high, low, cols_high[plane], cols_low[plane])

    @pl.when(plane == 0)
    def first():
        rows[step >> 1] = made

    @pl.when(plane == 1)
    def second():
        rows[step >> 1] += made

    @pl.when(step == 3)
    def finish():
        window = taper(iota((FS, 2 * SIDE * PART), 0))
        mixed = jnp.concatenate([rows[0] * window, rows[1] * window], axis=1)
        swapped = jnp.concatenate(
            [side for j in range(2) for side in (-mixed[:, j * 128 + 64 : j * 128 + 128], mixed[:, j * 128 : j * 128 + 64])],
            axis=1,
        )
        mixed_high, mixed_low = halves(mixed)
        swapped_high, swapped_low = halves(swapped)
        grid = mm3(table_high[0], table_low[0], mixed_high, mixed_low)
        grid += mm3(table_high[1], table_low[1], swapped_high, swapped_low)
        real, imag = quarter_turn(facet_row, facet_col)
        for a in range(SIDE):
            block = jnp.transpose(grid[a * XM : (a + 1) * XM])
            for b in range(SIDE):
                for j in range(2):
                    at = j * 128 + b * PART
                    re, im = block[at : at + PART], block[at + 64 : at + 64 + PART]
                    pieces[a * SIDE + b, j * 32 : j * 32 + 16] = real * re - imag * im
                    pieces[a * SIDE + b, j * 32 + 16 : j * 32 + 32] = real * im + imag * re
        for t in range(NF):
            out[t] = pieces[assignment[t]]


def misfit_kernel(contributions, visible, out, channel_of, tile_of):
    _, _, part = position()
    grids = contributions[0]
    for f in range(1, NF):
        grids = grids + contributions[f]
    high, low = halves(grids)
    stacked = jnp.concatenate([high, low], axis=0)
    total = jnp.int32(0)
    for c in range(CHANS):
        count = jnp.max(visible[c, META + 1 : META + 2, :]).astype(jnp.int32)
        for tile in range(TILES):

            @pl.when(tile * TILE < count)
            def note(c=c, tile=tile, total=total):
                channel_of[total + tile] = c
                tile_of[total + tile] = tile

        total = total + ((count + TILE - 1) >> 10)

    @pl.when((total & 1) == 1)
    def even():
        channel_of[total] = 0
        tile_of[total] = 0

    row_of = iota((XM, XM), 0)
    column_of = iota((2 * PART, XM), 0) & (PART - 1)

    def step(i, carry):
        sums = carry
        hots, scales = [], []
        wanted, seen = [], []
        for half in range(2):
            n = 2 * i + half
            c, tile = channel_of[n], tile_of[n]
            at = pl.multiple_of(tile * 8, 8)
            cells = visible[c, pl.ds(2 * ROWS + at, 8), :].astype(jnp.int32)
            cells = jnp.where(n < total, cells, -1)
            seen_re = visible[c, pl.ds(at, 8), :]
            seen_im = visible[c, pl.ds(ROWS + at, 8), :]
            scale = visible[c, META : META + 1, :]
            u, v = cells >> 7, (cells & (XM - 1)) - part * PART
            for r in range(8):
                hots.append(jnp.where(row_of == u[r : r + 1], 1.0, 0.0).astype(BF16))
                wanted.append(column_of == v[r : r + 1])
                seen.append(
                    jnp.concatenate(
                        [jnp.broadcast_to(seen_re[r : r + 1], (PART, XM)), jnp.broadcast_to(seen_im[r : r + 1], (PART, XM))], axis=0
                    )
                )
                scales.append(scale)
        hot = jnp.concatenate(hots, axis=1)
        found = mm(stacked, hot)
        found = found[:PIECE] + found[PIECE:]
        scale = jnp.concatenate(scales, axis=1)
        predicted = found[: 2 * PART] + scale * found[2 * PART :]
        missed = jnp.where(jnp.concatenate(wanted, axis=1), jnp.concatenate(seen, axis=1) - predicted, 0.0)
        missed = jnp.concatenate([missed, scale * missed], axis=0)
        missed_high, missed_low = halves(missed)
        return sums + mm(hot, jnp.concatenate([missed_high, missed_low], axis=0), ((1,), (1,)))

    sums = lax.fori_loop(0, (total + 1) >> 1, step, jnp.zeros((XM, 2 * PIECE), F32))
    turned = jnp.transpose(sums)
    result = turned[:PIECE] + turned[PIECE:]
    for f in range(NF):
        out[f] = result


def rows_kernel(assignment, pieces, table_high, table_low, out, placed):
    facet_row, facet_col, _ = position()
    real, imag = quarter_turn(facet_row, facet_col)
    for t in range(NF):
        s = assignment[t]
        for j in range(2):
            re, im = pieces[t, j * 32 : j * 32 + 16], pieces[t, j * 32 + 16 : j * 32 + 32]
            placed[s, j * 32 : j * 32 + 16] = real * re + imag * im
            placed[s, j * 32 + 16 : j * 32 + 32] = real * im - imag * re
    blocks = {}
    for j in range(2):
        for c in range(2):
            at = j * 32 + c * 16
            blocks[j, c] = jnp.concatenate(
                [jnp.concatenate([placed[a * SIDE + b, at : at + 16] for a in range(SIDE)], axis=1) for b in range(SIDE)], axis=0
            )
    grid = jnp.concatenate([blocks[0, 0], blocks[0, 1], blocks[1, 0], blocks[1, 1]], axis=0)
    swapped = jnp.concatenate([blocks[0, 1], -blocks[0, 0], blocks[1, 1], -blocks[1, 0]], axis=0)
    grid_high, grid_low = halves(grid)
    swapped_high, swapped_low = halves(swapped)
    both = ((1,), (1,))
    out[...] = mm3(table_high[0], table_low[0], grid_high, grid_low, both) + mm3(
        table_high[1], table_low[1], swapped_high, swapped_low, both
    )


def columns_kernel(mixed, table_high, table_low, out, perm_high, perm_low):
    _, _, part = position()
    for k in range(CHANS):
        for b in range(SIDE):
            to = slice(k * 64 + b * PART, k * 64 + (b + 1) * PART)
            frm = slice(b * XM + k * PART, b * XM + (k + 1) * PART)
            perm_high[:, to] = table_high[:, frm]
            perm_low[:, to] = table_low[:, frm]
    stripes = []
    for j in range(2):
        for c in range(2):
            at = j * 128 + c * 64
            stripes.append(jnp.concatenate([mixed[k, :, at : at + 64] for k in range(CHANS)], axis=1))
    high, low = halves(jnp.concatenate(stripes, axis=0))
    real = mm3(high, low, perm_high[0], perm_low[0])
    imag = mm3(high, low, perm_high[1], perm_low[1])
    shape = (64, FS)
    window = taper(iota(shape, 0) + part * 64) * taper(iota(shape, 1))
    for j in range(2):
        re, im = slice(j * 128, j * 128 + 64), slice(j * 128 + 64, j * 128 + 128)
        out[j, 0] = window * (real[re] + imag[im])
        out[j, 1] = window * (real[im] - imag[re])


def call(kernel, shapes, in_specs, scratch=(), **kwargs):
    return pl.pallas_call(
        kernel,
        out_shape=shapes,
        in_specs=in_specs,
        out_specs=jax.tree.map(lambda _: VMEM, shapes),
        scratch_shapes=list(scratch),
        **kwargs,
    )


def on_device(model_taylor, channel_offset, assignment, observed, uv_bins, vis_counts):
    message = call(pack_kernel, jax.ShapeDtypeStruct((CHANS, MSG, XM), F32), [SMEM, SMEM, VMEM, VMEM])(
        channel_offset, vis_counts, observed[0, 0], uv_bins[0]
    )
    visible = lax.all_to_all(message, "chan", 0, 0, tiled=True)

    table = jax.ShapeDtypeStruct((2, FS, FS), BF16)
    table_high, table_low, sent = pl.pallas_call(
        forward_kernel,
        out_shape=(table, table, jax.ShapeDtypeStruct((NF, PIECE, XM), F32)),
        grid=(4,),
        in_specs=[SMEM, pl.BlockSpec((1, 1, FS, FS), lambda i: (i // 2, i % 2, 0, 0))],
        out_specs=(
            pl.BlockSpec((2, FS, FS), lambda i: (0, 0, 0)),
            pl.BlockSpec((2, FS, FS), lambda i: (0, 0, 0)),
            pl.BlockSpec((NF, PIECE, XM), lambda i: (0, 0, 0)),
        ),
        scratch_shapes=[
            pltpu.VMEM((2, FS, 128), BF16),
            pltpu.VMEM((2, FS, 128), BF16),
            pltpu.VMEM((2, FS, 128), F32),
            pltpu.VMEM((NF, PIECE, XM), F32),
        ],
    )(assignment, model_taylor[:, 0])
    received = lax.all_to_all(sent, "facet", 0, 0, tiled=True)

    copies = call(
        misfit_kernel,
        jax.ShapeDtypeStruct((NF, PIECE, XM), F32),
        [VMEM, VMEM],
        [pltpu.SMEM((CHANS * TILES + 8,), jnp.int32), pltpu.SMEM((CHANS * TILES + 8,), jnp.int32)],
    )(received, visible)
    gathered = lax.all_to_all(copies, "facet", 0, 0, tiled=True)

    mixed = call(
        rows_kernel,
        jax.ShapeDtypeStruct((FS, 256), F32),
        [SMEM, VMEM, VMEM, VMEM],
        [pltpu.VMEM((NF, PIECE, XM), F32)],
    )(assignment, gathered, table_high, table_low)
    stripes = lax.all_to_all(mixed.reshape(CHANS, 64, 256), "chan", 0, 0, tiled=True)

    planes = call(
        columns_kernel,
        jax.ShapeDtypeStruct((2, 2, 64, FS), F32),
        [VMEM, VMEM, VMEM],
        [pltpu.VMEM((2, FS, FS), BF16), pltpu.VMEM((2, FS, FS), BF16)],
    )(stripes, table_high, table_low)
    return planes[:, None]


def solution(mesh):
    return jax.shard_map(
        on_device,
        mesh=mesh,
        in_specs=(
            P(None, "facet", None, None, None),
            P("chan"),
            P(),
            P("chan", "facet", None, None),
            P("chan", "facet", None),
            P("chan", "facet"),
        ),
        out_specs=P(None, "facet", None, "chan", None),
        check_vma=False,
    )
```

```python
import jax
import jax.numpy as jnp
from jax import lax
from jax.experimental import pallas as pl
from jax.experimental.pallas import tpu as pltpu
from jax.sharding import PartitionSpec as P


FS = 512
XM = 128
SIDE = 4
NF = 16
CHANS = 8
VIS = 4096
IMAGE = 2048
PART = XM // CHANS
PIECE = 4 * PART
ROWS = VIS // XM
META = 3 * ROWS
MSG = META + 8
TILE = 8 * XM
TILES = VIS // TILE
LISTED = 2 * CHANS * TILES + 8

LIMIT = 24 << 20
TURN = 6.283185307179586 / IMAGE
F32 = jnp.float32
BF16 = jnp.bfloat16
VMEM = pl.BlockSpec(memory_space=pltpu.VMEM)
SMEM = pl.BlockSpec(memory_space=pltpu.SMEM)
HBM = pl.BlockSpec(memory_space=pltpu.HBM)


def cos_turn(m):
    m = m & (IMAGE - 1)
    quarter = (m + 256) >> 9
    t = (m - (quarter << 9)).astype(F32) * TURN
    t2 = t * t
    even = 1.0 + t2 * (-0.5 + t2 * (1 / 24 + t2 * (-1 / 720 + t2 * (1 / 40320 - t2 * (1 / 3628800)))))
    odd = t * (1.0 + t2 * (-1 / 6 + t2 * (1 / 120 + t2 * (-1 / 5040 + t2 * (1 / 362880)))))
    value = jnp.where((quarter & 1) == 1, odd, even)
    return jnp.where(((quarter + 1) & 2) == 2, -value, value)


def taper(n):
    return (0.55 + 0.45 * cos_turn(4 * n - (2 * FS - 2))) * F32(1.0 / FS**0.5)


def halves(value):
    high = value.astype(BF16)
    return high, (value - high.astype(F32)).astype(BF16)


def iota(shape, dim):
    return lax.broadcasted_iota(jnp.int32, shape, dim)


def mm(a, b, dims=((1,), (0,))):
    return lax.dot_general(a, b, (dims, ((), ())), preferred_element_type=F32)


def mm3(a_high, a_low, b_high, b_low, dims=((1,), (0,))):
    return mm(a_high, b_high, dims) + (mm(a_high, b_low, dims) + mm(a_low, b_high, dims))


def position():
    facet = lax.axis_index("facet")
    return facet // SIDE, facet % SIDE, lax.axis_index("chan")


def quarter_turn(facet_row, facet_col):
    shape = (PART, XM)
    turn = (iota(shape, 1) * facet_row + iota(shape, 0) * facet_col) & 3
    real = jnp.where(turn == 0, 1.0, jnp.where(turn == 2, -1.0, 0.0)).astype(F32)
    imag = jnp.where(turn == 3, 1.0, jnp.where(turn == 1, -1.0, 0.0)).astype(F32)
    return real, imag


def forward_kernel(
    offset, count, assignment, sky, observed, bins, table_high, table_low, out, message,
    image, seen, cells, offset_here, count_here, order, cols_high, cols_low, rows, pieces, arrived,
):
    facet_row, facet_col, part = position()
    small = [
        pltpu.make_async_copy(frm, to, arrived.at[n])
        for n, (frm, to) in enumerate(
            ((offset, offset_here), (count, count_here), (assignment, order), (observed, seen), (bins, cells))
        )
    ]
    planes = [pltpu.make_async_copy(sky.at[n // 2, n % 2], image.at[n], arrived.at[5 + n]) for n in range(4)]
    for copy in planes + small:
        copy.start()

    pixel = iota((PART, FS), 1)
    fine = iota((PART, FS), 0) * pixel
    fine_re, fine_im = cos_turn(fine), cos_turn(fine + 512)
    coarse = iota((FS // PART, FS), 0) * PART * iota((FS // PART, FS), 1)
    coarse_re, coarse_im = cos_turn(coarse), cos_turn(coarse + 512)
    for g in range(FS // PART):
        re, im = coarse_re[g : g + 1], coarse_im[g : g + 1]
        here = slice(g * PART, (g + 1) * PART)
        table_high[0, here], table_low[0, here] = halves(re * fine_re - im * fine_im)
        table_high[1, here], table_low[1, here] = halves(re * fine_im + im * fine_re)
    shape = (FS, 2 * SIDE * PART)
    y, lane = iota(shape, 0), iota(shape, 1)
    column = ((lane & 63) >> 4) * XM + part * PART + (lane & (PART - 1))
    turn = column * y + jnp.where(lane >= 64, 512, 0)
    window = taper(y)
    cols_high[0], cols_low[0] = halves(cos_turn(turn) * window)
    cols_high[1], cols_low[1] = halves(cos_turn(turn - 512) * window)

    for n in range(4):
        planes[n].wait()
        high, low = halves(image[n])
        both = mm(high, jnp.concatenate([cols_high[n % 2], cols_low[n % 2]], axis=1))
        made = both[:, :128] + (both[:, 128:] + mm(low, cols_high[n % 2]))
        if n % 2 == 0:
            rows[n // 2] = made
        else:
            rows[n // 2] += made

    for copy in small:
        copy.wait()
    live = iota((1, VIS), 1) < count_here[0, 0]
    marked = jnp.where(live, cells[...].astype(F32), -1.0)
    for row in range(ROWS):
        lanes = slice(row * XM, (row + 1) * XM)
        message[row : row + 1, :] = seen[0:1, lanes]
        message[ROWS + row : ROWS + row + 1, :] = seen[1:2, lanes]
        message[2 * ROWS + row : 2 * ROWS + row + 1, :] = marked[:, lanes]
    place = iota((8, XM), 0)
    meta = jnp.where(place == 0, offset_here[0], jnp.where(place == 1, count_here[0, 0].astype(F32), 0.0))
    message[META:MSG, :] = meta

    mixed = jnp.concatenate([rows[0] * window, rows[1] * window], axis=1)
    swapped = jnp.concatenate(
        [side for j in range(2) for side in (-mixed[:, j * 128 + 64 : j * 128 + 128], mixed[:, j * 128 : j * 128 + 64])],
        axis=1,
    )
    mixed_high, mixed_low = halves(mixed)
    swapped_high, swapped_low = halves(swapped)
    real, imag = quarter_turn(facet_row, facet_col)
    for a in range(SIDE):
        here = slice(a * XM, (a + 1) * XM)
        grid = mm3(table_high[0, here], table_low[0, here], mixed_high, mixed_low)
        grid += mm3(table_high[1, here], table_low[1, here], swapped_high, swapped_low)
        block = jnp.transpose(grid)
        for b in range(SIDE):
            for j in range(2):
                at = j * 128 + b * PART
                re, im = block[at : at + PART], block[at + 64 : at + 64 + PART]
                pieces[a * SIDE + b, j * 32 : j * 32 + 16] = real * re - imag * im
                pieces[a * SIDE + b, j * 32 + 16 : j * 32 + 32] = real * im + imag * re
    for t in range(NF):
        out[t] = pieces[order[t]]


def tiles_kernel(*refs):
    *visible, listed = refs
    total = jnp.int32(0)
    for c in range(CHANS):
        count = jnp.max(visible[c][META + 1 : META + 2, :]).astype(jnp.int32)
        for tile in range(TILES):

            @pl.when(tile * TILE < count)
            def note(c=c, tile=tile, total=total):
                listed[2 * (total + tile)] = c
                listed[2 * (total + tile) + 1] = tile

        total = total + ((count + TILE - 1) >> 10)

    @pl.when((total & 1) == 1)
    def even():
        listed[2 * total] = 0
        listed[2 * total + 1] = 0

    listed[LISTED - 1] = total


def misfit_kernel(contributions, listed, *refs):
    *visible, out = refs
    _, _, part = position()
    grids = contributions[0]
    for f in range(1, NF):
        grids = grids + contributions[f]
    high, low = halves(grids)
    stacked = jnp.concatenate([high, low], axis=0)
    total = listed[LISTED - 1]
    row_of = iota((XM, XM), 0)
    column_of = iota((2 * PART, XM), 0) & (PART - 1)

    def step(i, carry):
        sums = carry
        hots, scales = [], []
        wanted, seen = [], []
        for half in range(2):
            n = 2 * i + half
            c, tile = listed[2 * n], listed[2 * n + 1]
            at = pl.multiple_of(tile * 8, 8)

            def of_channel(start, size, c=c):
                found = visible[0][pl.ds(start, size), :]
                for other in range(1, CHANS):
                    found = jnp.where(c == other, visible[other][pl.ds(start, size), :], found)
                return found

            cells = of_channel(2 * ROWS + at, 8).astype(jnp.int32)
            cells = jnp.where(n < total, cells, -1)
            seen_re = of_channel(at, 8)
            seen_im = of_channel(ROWS + at, 8)
            scale = of_channel(META, 1)
            u, v = cells >> 7, (cells & (XM - 1)) - part * PART
            for r in range(8):
                hots.append(jnp.where(row_of == u[r : r + 1], 1.0, 0.0).astype(BF16))
                wanted.append(column_of == v[r : r + 1])
                seen.append(
                    jnp.concatenate(
                        [jnp.broadcast_to(seen_re[r : r + 1], (PART, XM)), jnp.broadcast_to(seen_im[r : r + 1], (PART, XM))], axis=0
                    )
                )
                scales.append(scale)
        hot = jnp.concatenate(hots, axis=1)
        found = mm(stacked, hot)
        found = found[:PIECE] + found[PIECE:]
        scale = jnp.concatenate(scales, axis=1)
        predicted = found[: 2 * PART] + scale * found[2 * PART :]
        missed = jnp.where(jnp.concatenate(wanted, axis=1), jnp.concatenate(seen, axis=1) - predicted, 0.0)
        missed = jnp.concatenate([missed, scale * missed], axis=0)
        missed_high, missed_low = halves(missed)
        return sums + mm(hot, jnp.concatenate([missed_high, missed_low], axis=0), ((1,), (1,)))

    sums = lax.fori_loop(0, (total + 1) >> 1, step, jnp.zeros((XM, 2 * PIECE), F32))
    turned = jnp.transpose(sums)
    result = turned[:PIECE] + turned[PIECE:]
    for f in range(NF):
        out[f] = result


def rows_kernel(assignment, pieces, table_high, table_low, out, placed):
    facet_row, facet_col, _ = position()
    real, imag = quarter_turn(facet_row, facet_col)
    for t in range(NF):
        s = assignment[t]
        for j in range(2):
            re, im = pieces[t, j * 32 : j * 32 + 16], pieces[t, j * 32 + 16 : j * 32 + 32]
            placed[s, j * 32 : j * 32 + 16] = real * re + imag * im
            placed[s, j * 32 + 16 : j * 32 + 32] = real * im - imag * re
    blocks = {}
    for j in range(2):
        for c in range(2):
            at = j * 32 + c * 16
            blocks[j, c] = jnp.concatenate(
                [jnp.concatenate([placed[a * SIDE + b, at : at + 16] for a in range(SIDE)], axis=1) for b in range(SIDE)], axis=0
            )
    grid = jnp.concatenate([blocks[0, 0], blocks[0, 1], blocks[1, 0], blocks[1, 1]], axis=0)
    swapped = jnp.concatenate([blocks[0, 1], -blocks[0, 0], blocks[1, 1], -blocks[1, 0]], axis=0)
    grid_high, grid_low = halves(grid)
    swapped_high, swapped_low = halves(swapped)
    both = ((1,), (1,))
    out[...] = mm3(table_high[0], table_low[0], grid_high, grid_low, both) + mm3(
        table_high[1], table_low[1], swapped_high, swapped_low, both
    )


def columns_kernel(mixed, table_high, table_low, out, perm_high, perm_low):
    _, _, part = position()
    for k in range(CHANS):
        for b in range(SIDE):
            to = slice(k * 64 + b * PART, k * 64 + (b + 1) * PART)
            frm = slice(b * XM + k * PART, b * XM + (k + 1) * PART)
            perm_high[:, to] = table_high[:, frm]
            perm_low[:, to] = table_low[:, frm]
    stripes = []
    for j in range(2):
        for c in range(2):
            at = j * 128 + c * 64
            stripes.append(jnp.concatenate([mixed[k, :, at : at + 64] for k in range(CHANS)], axis=1))
    high, low = halves(jnp.concatenate(stripes, axis=0))
    real = mm3(high, low, perm_high[0], perm_low[0])
    imag = mm3(high, low, perm_high[1], perm_low[1])
    shape = (64, FS)
    window = taper(iota(shape, 0) + part * 64) * taper(iota(shape, 1))
    for j in range(2):
        re, im = slice(j * 128, j * 128 + 64), slice(j * 128 + 64, j * 128 + 128)
        out[j, 0] = window * (real[re] + imag[im])
        out[j, 1] = window * (real[im] - imag[re])


def call(kernel, shapes, in_specs, scratch=(), **kwargs):
    return pl.pallas_call(
        kernel,
        out_shape=shapes,
        in_specs=in_specs,
        out_specs=jax.tree.map(lambda _: VMEM, shapes),
        scratch_shapes=list(scratch),
        compiler_params=pltpu.CompilerParams(vmem_limit_bytes=LIMIT),
        **kwargs,
    )


def on_device(model_taylor, channel_offset, assignment, observed, uv_bins, vis_counts):
    table = jax.ShapeDtypeStruct((2, FS, FS), BF16)
    table_high, table_low, sent, message = call(
        forward_kernel,
        (table, table, jax.ShapeDtypeStruct((NF, PIECE, XM), F32), jax.ShapeDtypeStruct((MSG, XM), F32)),
        [HBM] * 6,
        [
            pltpu.VMEM((4, FS, FS), F32),
            pltpu.VMEM((2, VIS), F32),
            pltpu.VMEM((1, VIS), jnp.int32),
            pltpu.SMEM((1,), F32),
            pltpu.SMEM((1, 1), jnp.int32),
            pltpu.SMEM((NF,), jnp.int32),
            pltpu.VMEM((2, FS, 128), BF16),
            pltpu.VMEM((2, FS, 128), BF16),
            pltpu.VMEM((2, FS, 128), F32),
            pltpu.VMEM((NF, PIECE, XM), F32),
            pltpu.SemaphoreType.DMA((9,)),
        ],
    )(channel_offset, vis_counts, *(pltpu.with_memory_space_constraint(x, pltpu.HBM) for x in (assignment, model_taylor[:, 0], observed[0, 0], uv_bins[0])))
    received = lax.all_to_all(sent, "facet", 0, 0, tiled=True)
    own = [message] + [lax.ppermute(message, "chan", [(c, (c + 2 * d) % CHANS) for c in range(CHANS)]) for d in (1, 2, 3)]
    visible = own + [lax.ppermute(piece, "chan", [(c, c ^ 1) for c in range(CHANS)]) for piece in own]
    listed = pl.pallas_call(
        tiles_kernel,
        out_shape=jax.ShapeDtypeStruct((LISTED,), jnp.int32),
        in_specs=[VMEM] * CHANS,
        out_specs=SMEM,
        compiler_params=pltpu.CompilerParams(vmem_limit_bytes=LIMIT),
    )(*visible)
    copies = call(misfit_kernel, jax.ShapeDtypeStruct((NF, PIECE, XM), F32), [VMEM, SMEM] + [VMEM] * CHANS)(
        received, listed, *visible
    )
    gathered = lax.all_to_all(copies, "facet", 0, 0, tiled=True)

    mixed = call(
        rows_kernel,
        jax.ShapeDtypeStruct((FS, 256), F32),
        [SMEM, VMEM, VMEM, VMEM],
        [pltpu.VMEM((NF, PIECE, XM), F32)],
    )(assignment, gathered, table_high, table_low)
    stripes = lax.all_to_all(mixed.reshape(CHANS, 64, 256), "chan", 0, 0, tiled=True)

    planes = call(
        columns_kernel,
        jax.ShapeDtypeStruct((2, 2, 64, FS), F32),
        [VMEM, VMEM, VMEM],
        [pltpu.VMEM((2, FS, FS), BF16), pltpu.VMEM((2, FS, FS), BF16)],
    )(stripes, table_high, table_low)
    return planes[:, None]


def solution(mesh):
    return jax.shard_map(
        on_device,
        mesh=mesh,
        in_specs=(
            P(None, "facet", None, None, None),
            P("chan"),
            P(),
            P("chan", "facet", None, None),
            P("chan", "facet", None),
            P("chan", "facet"),
        ),
        out_specs=P(None, "facet", None, "chan", None),
        check_vma=False,
    )
```

```python
import jax
import jax.numpy as jnp
from jax import lax
from jax.experimental import pallas as pl
from jax.experimental.pallas import tpu as pltpu
from jax.sharding import PartitionSpec as P


FS = 512
XM = 128
SIDE = 4
NF = 16
CHANS = 8
VIS = 4096
IMAGE = 2048
PART = XM // CHANS
PIECE = 4 * PART
ROWS = VIS // XM
META = 3 * ROWS
MSG = META + 8
GROUP = 16

LIMIT = 24 << 20
TURN = 6.283185307179586 / IMAGE
F32 = jnp.float32
BF16 = jnp.bfloat16
VMEM = pl.BlockSpec(memory_space=pltpu.VMEM)
SMEM = pl.BlockSpec(memory_space=pltpu.SMEM)
HBM = pl.BlockSpec(memory_space=pltpu.HBM)


def cos_turn(m):
    m = m & (IMAGE - 1)
    quarter = (m + 256) >> 9
    t = (m - (quarter << 9)).astype(F32) * TURN
    t2 = t * t
    even = 1.0 + t2 * (-0.5 + t2 * (1 / 24 + t2 * (-1 / 720 + t2 * (1 / 40320 - t2 * (1 / 3628800)))))
    odd = t * (1.0 + t2 * (-1 / 6 + t2 * (1 / 120 + t2 * (-1 / 5040 + t2 * (1 / 362880)))))
    value = jnp.where((quarter & 1) == 1, odd, even)
    return jnp.where(((quarter + 1) & 2) == 2, -value, value)


def taper(n):
    return (0.55 + 0.45 * cos_turn(4 * n - (2 * FS - 2))) * F32(1.0 / FS**0.5)


def halves(value):
    high = value.astype(BF16)
    return high, (value - high.astype(F32)).astype(BF16)


def iota(shape, dim):
    return lax.broadcasted_iota(jnp.int32, shape, dim)


def mm(a, b, dims=((1,), (0,))):
    return lax.dot_general(a, b, (dims, ((), ())), preferred_element_type=F32)


def mm3(a_high, a_low, b_high, b_low, dims=((1,), (0,))):
    return mm(a_high, b_high, dims) + (mm(a_high, b_low, dims) + mm(a_low, b_high, dims))


def position():
    facet = lax.axis_index("facet")
    return facet // SIDE, facet % SIDE, lax.axis_index("chan")


def quarter_turn(facet_row, facet_col):
    shape = (PART, XM)
    turn = (iota(shape, 1) * facet_row + iota(shape, 0) * facet_col) & 3
    real = jnp.where(turn == 0, 1.0, jnp.where(turn == 2, -1.0, 0.0)).astype(F32)
    imag = jnp.where(turn == 3, 1.0, jnp.where(turn == 1, -1.0, 0.0)).astype(F32)
    return real, imag


def forward_kernel(
    offset, count, assignment, sky, observed, bins, table_high, table_low, out, message,
    image, seen, cells, offset_here, count_here, order, cols_high, cols_low, rows, pieces, arrived,
):
    facet_row, facet_col, part = position()
    small = [
        pltpu.make_async_copy(frm, to, arrived.at[n])
        for n, (frm, to) in enumerate(
            ((offset, offset_here), (count, count_here), (assignment, order), (observed, seen), (bins, cells))
        )
    ]
    planes = [pltpu.make_async_copy(sky.at[n // 2, n % 2], image.at[n], arrived.at[5 + n]) for n in range(4)]
    for copy in planes + small:
        copy.start()

    lane = iota((PART, XM), 1)
    column = ((lane & 63) >> 4) * XM + part * PART + (lane & (PART - 1))
    side = jnp.where(lane >= 64, 512, 0)
    fine_y = column * iota((PART, XM), 0) + side
    fine_one, fine_two = cos_turn(fine_y), cos_turn(fine_y + 512)
    lane = iota((FS // PART, XM), 1)
    column = ((lane & 63) >> 4) * XM + part * PART + (lane & (PART - 1))
    coarse_y = column * PART * iota((FS // PART, XM), 0)
    coarse_re, coarse_im = cos_turn(coarse_y), cos_turn(coarse_y + 512)
    window = jnp.transpose(jnp.broadcast_to(taper(iota((1, FS), 1)), (XM, FS)))
    for g in range(FS // PART):
        here = slice(g * PART, (g + 1) * PART)
        re, im = coarse_re[g : g + 1] * window[here], coarse_im[g : g + 1] * window[here]
        cols_high[0, here], cols_low[0, here] = halves(re * fine_one - im * fine_two)
        cols_high[1, here], cols_low[1, here] = halves(-(im * fine_one + re * fine_two))

    fine = iota((PART, FS), 0) * iota((PART, FS), 1)
    fine_re, fine_im = cos_turn(fine), cos_turn(fine + 512)
    coarse = iota((FS // PART, FS), 0) * PART * iota((FS // PART, FS), 1)
    coarse_re, coarse_im = cos_turn(coarse), cos_turn(coarse + 512)

    for n in range(4):
        planes[n].wait()
        high, low = halves(image[n])
        both = mm(high, jnp.concatenate([cols_high[n % 2], cols_low[n % 2]], axis=1))
        made = both[:, :128] + (both[:, 128:] + mm(low, cols_high[n % 2]))
        if n % 2 == 0:
            rows[n // 2] = made
        else:
            rows[n // 2] += made
        for g in range(8 * n, 8 * n + 8):
            re, im = coarse_re[g : g + 1], coarse_im[g : g + 1]
            here = slice(g * PART, (g + 1) * PART)
            table_high[0, here], table_low[0, here] = halves(re * fine_re - im * fine_im)
            table_high[1, here], table_low[1, here] = halves(re * fine_im + im * fine_re)

    for copy in small:
        copy.wait()
    live = iota((1, VIS), 1) < count_here[0, 0]
    marked = jnp.where(live, cells[...].astype(F32), -1.0)
    for row in range(ROWS):
        lanes = slice(row * XM, (row + 1) * XM)
        message[row : row + 1, :] = seen[0:1, lanes]
        message[ROWS + row : ROWS + row + 1, :] = seen[1:2, lanes]
        message[2 * ROWS + row : 2 * ROWS + row + 1, :] = marked[:, lanes]
    place = iota((8, XM), 0)
    meta = jnp.where(place == 0, offset_here[0], jnp.where(place == 1, count_here[0, 0].astype(F32), 0.0))
    message[META:MSG, :] = meta

    mixed = jnp.concatenate([rows[0] * window, rows[1] * window], axis=1)
    swapped = jnp.concatenate(
        [side for j in range(2) for side in (-mixed[:, j * 128 + 64 : j * 128 + 128], mixed[:, j * 128 : j * 128 + 64])],
        axis=1,
    )
    mixed_high, mixed_low = halves(mixed)
    swapped_high, swapped_low = halves(swapped)
    real, imag = quarter_turn(facet_row, facet_col)
    for a in range(SIDE):
        here = slice(a * XM, (a + 1) * XM)
        grid = mm3(table_high[0, here], table_low[0, here], mixed_high, mixed_low)
        grid += mm3(table_high[1, here], table_low[1, here], swapped_high, swapped_low)
        block = jnp.transpose(grid)
        for b in range(SIDE):
            for j in range(2):
                at = j * 128 + b * PART
                re, im = block[at : at + PART], block[at + 64 : at + 64 + PART]
                pieces[a * SIDE + b, j * 32 : j * 32 + 16] = real * re - imag * im
                pieces[a * SIDE + b, j * 32 + 16 : j * 32 + 32] = real * im + imag * re
    for t in range(NF):
        out[t] = pieces[order[t]]


def misfit_kernel(contributions, *refs):
    *visible, out, sums = refs
    _, _, part = position()
    grids = contributions[0]
    for f in range(1, NF):
        grids = grids + contributions[f]
    row_of = [(iota((PART, XM), 0) + g * PART).astype(F32).astype(BF16) for g in range(XM // PART)]
    column_of = iota((2 * PART, XM), 0) & (PART - 1)
    one, zero = jnp.ones((PART, XM), BF16), jnp.zeros((PART, XM), BF16)

    def slots(c, first):
        seen, scale = visible[c], visible[c][META : META + 1]
        grid_high, grid_low = halves(grids[: 2 * PART] + scale * grids[2 * PART :])
        cells = seen[2 * ROWS + first : 2 * ROWS + first + GROUP].astype(jnp.int32)
        u, v = (cells >> 7).astype(F32), (cells & (XM - 1)) - part * PART
        hots, misses = [], []
        for r in range(GROUP):
            u_here = jnp.broadcast_to(u[r : r + 1], (PART, XM)).astype(BF16)
            hots.append(jnp.concatenate([jnp.where(rows == u_here, one, zero) for rows in row_of], axis=0))
        hot = jnp.concatenate(hots, axis=1)
        found = mm(jnp.concatenate([grid_high, grid_low], axis=0), hot)
        predicted = found[: 2 * PART] + found[2 * PART :]
        for r in range(GROUP):
            re = jnp.broadcast_to(seen[first + r : first + r + 1], (PART, XM))
            im = jnp.broadcast_to(seen[ROWS + first + r : ROWS + first + r + 1], (PART, XM))
            missed = jnp.concatenate([re, im], axis=0) - predicted[:, r * XM : (r + 1) * XM]
            misses.append(jnp.where(column_of == v[r : r + 1], missed, 0.0))
        missed = jnp.concatenate(halves(jnp.concatenate(misses, axis=1)), axis=0)
        return mm(hot, missed, ((1,), (1,))), scale[:, :PIECE]

    totals = [jnp.zeros((XM, PIECE), F32)] * 2
    for c in range(CHANS):
        made, scale = slots(c, 0)
        totals = [totals[0] + made, totals[1] + scale * made]
    sums[0], sums[1] = totals
    for first in range(GROUP, ROWS, GROUP):
        for c in range(CHANS):

            @pl.when(jnp.max(visible[c][META + 1 : META + 2]) > first * XM)
            def more(c=c, first=first):
                made, scale = slots(c, first)
                sums[0] += made
                sums[1] += scale * made

    turned = jnp.transpose(jnp.concatenate([sums[0], sums[1]], axis=1))
    result = jnp.concatenate([turned[0:32] + turned[32:64], turned[64:96] + turned[96:128]], axis=0)
    for f in range(NF):
        out[f] = result


def rows_kernel(assignment, pieces, table_high, table_low, out, placed):
    facet_row, facet_col, _ = position()
    real, imag = quarter_turn(facet_row, facet_col)
    for t in range(NF):
        s = assignment[t]
        for j in range(2):
            re, im = pieces[t, j * 32 : j * 32 + 16], pieces[t, j * 32 + 16 : j * 32 + 32]
            placed[s, j * 32 : j * 32 + 16] = real * re + imag * im
            placed[s, j * 32 + 16 : j * 32 + 32] = real * im - imag * re
    blocks = {}
    for j in range(2):
        for c in range(2):
            at = j * 32 + c * 16
            blocks[j, c] = jnp.concatenate(
                [jnp.concatenate([placed[a * SIDE + b, at : at + 16] for a in range(SIDE)], axis=1) for b in range(SIDE)], axis=0
            )
    grid = jnp.concatenate([blocks[0, 0], blocks[0, 1], blocks[1, 0], blocks[1, 1]], axis=0)
    swapped = jnp.concatenate([blocks[0, 1], -blocks[0, 0], blocks[1, 1], -blocks[1, 0]], axis=0)
    grid_high, grid_low = halves(grid)
    swapped_high, swapped_low = halves(swapped)
    both = ((1,), (1,))
    out[...] = mm3(table_high[0], table_low[0], grid_high, grid_low, both) + mm3(
        table_high[1], table_low[1], swapped_high, swapped_low, both
    )


def columns_kernel(mixed, table_high, table_low, out, perm_high, perm_low):
    _, _, part = position()
    for k in range(CHANS):
        for b in range(SIDE):
            to = slice(k * 64 + b * PART, k * 64 + (b + 1) * PART)
            frm = slice(b * XM + k * PART, b * XM + (k + 1) * PART)
            perm_high[:, to] = table_high[:, frm]
            perm_low[:, to] = table_low[:, frm]
    stripes = []
    for j in range(2):
        for c in range(2):
            at = j * 128 + c * 64
            stripes.append(jnp.concatenate([mixed[k, :, at : at + 64] for k in range(CHANS)], axis=1))
    high, low = halves(jnp.concatenate(stripes, axis=0))
    real = mm3(high, low, perm_high[0], perm_low[0])
    imag = mm3(high, low, perm_high[1], perm_low[1])
    window = jnp.concatenate([taper(iota((64, XM), 0) + part * 64)] * (FS // XM), axis=1) * taper(iota((1, FS), 1))
    for j in range(2):
        re, im = slice(j * 128, j * 128 + 64), slice(j * 128 + 64, j * 128 + 128)
        out[j, 0] = window * (real[re] + imag[im])
        out[j, 1] = window * (real[im] - imag[re])


def call(kernel, shapes, in_specs, scratch=(), **kwargs):
    return pl.pallas_call(
        kernel,
        out_shape=shapes,
        in_specs=in_specs,
        out_specs=jax.tree.map(lambda _: VMEM, shapes),
        scratch_shapes=list(scratch),
        compiler_params=pltpu.CompilerParams(vmem_limit_bytes=LIMIT),
        **kwargs,
    )


def on_device(model_taylor, channel_offset, assignment, observed, uv_bins, vis_counts):
    table = jax.ShapeDtypeStruct((2, FS, FS), BF16)
    table_high, table_low, sent, message = call(
        forward_kernel,
        (table, table, jax.ShapeDtypeStruct((NF, PIECE, XM), F32), jax.ShapeDtypeStruct((MSG, XM), F32)),
        [HBM] * 6,
        [
            pltpu.VMEM((4, FS, FS), F32),
            pltpu.VMEM((2, VIS), F32),
            pltpu.VMEM((1, VIS), jnp.int32),
            pltpu.SMEM((1,), F32),
            pltpu.SMEM((1, 1), jnp.int32),
            pltpu.SMEM((NF,), jnp.int32),
            pltpu.VMEM((2, FS, 128), BF16),
            pltpu.VMEM((2, FS, 128), BF16),
            pltpu.VMEM((2, FS, 128), F32),
            pltpu.VMEM((NF, PIECE, XM), F32),
            pltpu.SemaphoreType.DMA((9,)),
        ],
    )(channel_offset, vis_counts, *(pltpu.with_memory_space_constraint(x, pltpu.HBM) for x in (assignment, model_taylor[:, 0], observed[0, 0], uv_bins[0])))
    received = lax.all_to_all(sent, "facet", 0, 0, tiled=True)
    own = [message] + [lax.ppermute(message, "chan", [(c, (c + 2 * d) % CHANS) for c in range(CHANS)]) for d in (1, 2, 3)]
    visible = own + [lax.ppermute(piece, "chan", [(c, c ^ 1) for c in range(CHANS)]) for piece in own]
    copies = call(
        misfit_kernel,
        jax.ShapeDtypeStruct((NF, PIECE, XM), F32),
        [VMEM] * (1 + CHANS),
        [pltpu.VMEM((2, XM, PIECE), F32)],
    )(received, *visible)
    gathered = lax.all_to_all(copies, "facet", 0, 0, tiled=True)

    mixed = call(
        rows_kernel,
        jax.ShapeDtypeStruct((FS, 256), F32),
        [SMEM, VMEM, VMEM, VMEM],
        [pltpu.VMEM((NF, PIECE, XM), F32)],
    )(assignment, gathered, table_high, table_low)
    stripes = lax.all_to_all(mixed.reshape(CHANS, 64, 256), "chan", 0, 0, tiled=True)

    planes = call(
        columns_kernel,
        jax.ShapeDtypeStruct((2, 2, 64, FS), F32),
        [VMEM, VMEM, VMEM],
        [pltpu.VMEM((2, FS, FS), BF16), pltpu.VMEM((2, FS, FS), BF16)],
    )(stripes, table_high, table_low)
    return planes[:, None]


def solution(mesh):
    return jax.shard_map(
        on_device,
        mesh=mesh,
        in_specs=(
            P(None, "facet", None, None, None),
            P("chan"),
            P(),
            P("chan", "facet", None, None),
            P("chan", "facet", None),
            P("chan", "facet"),
        ),
        out_specs=P(None, "facet", None, "chan", None),
        check_vma=False,
    )
```

```python
import jax
import jax.numpy as jnp
from jax import lax
from jax.experimental import pallas as pl
from jax.experimental.pallas import tpu as pltpu
from jax.sharding import PartitionSpec as P


FS = 512
XM = 128
SIDE = 4
NF = 16
CHANS = 8
VIS = 4096
IMAGE = 2048
PART = XM // CHANS
PIECE = 4 * PART
ROWS = VIS // XM
META = 3 * ROWS
MSG = META + 8
GROUP = 16

LIMIT = 24 << 20
TURN = 6.283185307179586 / IMAGE
F32 = jnp.float32
BF16 = jnp.bfloat16
VMEM = pl.BlockSpec(memory_space=pltpu.VMEM)
SMEM = pl.BlockSpec(memory_space=pltpu.SMEM)
HBM = pl.BlockSpec(memory_space=pltpu.HBM)


def cos_turn(m):
    m = m & (IMAGE - 1)
    quarter = (m + 256) >> 9
    t = (m - (quarter << 9)).astype(F32) * TURN
    t2 = t * t
    even = 1.0 + t2 * (-0.5 + t2 * (1 / 24 + t2 * (-1 / 720 + t2 * (1 / 40320 - t2 * (1 / 3628800)))))
    odd = t * (1.0 + t2 * (-1 / 6 + t2 * (1 / 120 + t2 * (-1 / 5040 + t2 * (1 / 362880)))))
    value = jnp.where((quarter & 1) == 1, odd, even)
    return jnp.where(((quarter + 1) & 2) == 2, -value, value)


def taper(n):
    return (0.55 + 0.45 * cos_turn(4 * n - (2 * FS - 2))) * F32(1.0 / FS**0.5)


def halves(value):
    high = value.astype(BF16)
    return high, (value - high.astype(F32)).astype(BF16)


def iota(shape, dim):
    return lax.broadcasted_iota(jnp.int32, shape, dim)


def mm(a, b, dims=((1,), (0,))):
    return lax.dot_general(a, b, (dims, ((), ())), preferred_element_type=F32)


def mm3(a_high, a_low, b_high, b_low, dims=((1,), (0,))):
    return mm(a_high, b_high, dims) + (mm(a_high, b_low, dims) + mm(a_low, b_high, dims))


def position():
    facet = lax.axis_index("facet")
    return facet // SIDE, facet % SIDE, lax.axis_index("chan")


def quarter_turn(facet_row, facet_col):
    shape = (PART, XM)
    turn = (iota(shape, 1) * facet_row + iota(shape, 0) * facet_col) & 3
    real = jnp.where(turn == 0, 1.0, jnp.where(turn == 2, -1.0, 0.0)).astype(F32)
    imag = jnp.where(turn == 3, 1.0, jnp.where(turn == 1, -1.0, 0.0)).astype(F32)
    return real, imag


def forward_kernel(
    offset, count, assignment, sky, observed, bins, table_high, table_low, out, message,
    image, seen, cells, offset_here, count_here, order, task_of, cols_high, cols_low, rows, pieces, arrived, left,
):
    facet_row, facet_col, part = position()
    small = [
        pltpu.make_async_copy(frm, to, arrived.at[n])
        for n, (frm, to) in enumerate(
            ((offset, offset_here), (count, count_here), (assignment, order), (observed, seen), (bins, cells))
        )
    ]
    planes = [pltpu.make_async_copy(sky.at[n // 2, n % 2], image.at[n], arrived.at[5 + n]) for n in range(4)]
    for copy in planes + small:
        copy.start()

    lane = iota((PART, XM), 1)
    column = ((lane & 63) >> 4) * XM + part * PART + (lane & (PART - 1))
    side = jnp.where(lane >= 64, 512, 0)
    fine_y = column * iota((PART, XM), 0) + side
    fine_one, fine_two = cos_turn(fine_y), cos_turn(fine_y + 512)
    lane = iota((FS // PART, XM), 1)
    column = ((lane & 63) >> 4) * XM + part * PART + (lane & (PART - 1))
    coarse_y = column * PART * iota((FS // PART, XM), 0)
    coarse_re, coarse_im = cos_turn(coarse_y), cos_turn(coarse_y + 512)
    window = jnp.transpose(jnp.broadcast_to(taper(iota((1, FS), 1)), (XM, FS)))
    for g in range(FS // PART):
        here = slice(g * PART, (g + 1) * PART)
        re, im = coarse_re[g : g + 1] * window[here], coarse_im[g : g + 1] * window[here]
        cols_high[0, here], cols_low[0, here] = halves(re * fine_one - im * fine_two)
        cols_high[1, here], cols_low[1, here] = halves(-(im * fine_one + re * fine_two))

    fine = iota((PART, FS), 0) * iota((PART, FS), 1)
    fine_re, fine_im = cos_turn(fine), cos_turn(fine + 512)
    coarse = iota((FS // PART, FS), 0) * PART * iota((FS // PART, FS), 1)
    coarse_re, coarse_im = cos_turn(coarse), cos_turn(coarse + 512)

    for g in range(FS // PART):
        re, im = coarse_re[g : g + 1], coarse_im[g : g + 1]
        here = slice(g * PART, (g + 1) * PART)
        table_high[0, here], table_low[0, here] = halves(re * fine_re - im * fine_im)
        table_high[1, here], table_low[1, here] = halves(re * fine_im + im * fine_re)

    for n in range(4):
        planes[n].wait()
        high, low = halves(image[n])
        both = mm(high, jnp.concatenate([cols_high[n % 2], cols_low[n % 2]], axis=1))
        made = both[:, :128] + (both[:, 128:] + mm(low, cols_high[n % 2]))
        if n % 2 == 0:
            rows[n // 2] = made
        else:
            rows[n // 2] += made

    for copy in small:
        copy.wait()
    for t in range(NF):
        task_of[order[t]] = t
    live = iota((1, VIS), 1) < count_here[0, 0]
    marked = jnp.where(live, cells[...].astype(F32), -1.0)
    for row in range(ROWS):
        lanes = slice(row * XM, (row + 1) * XM)
        message[row : row + 1, :] = seen[0:1, lanes]
        message[ROWS + row : ROWS + row + 1, :] = seen[1:2, lanes]
        message[2 * ROWS + row : 2 * ROWS + row + 1, :] = marked[:, lanes]
    place = iota((8, XM), 0)
    meta = jnp.where(place == 0, offset_here[0], jnp.where(place == 1, count_here[0, 0].astype(F32), 0.0))
    message[META:MSG, :] = meta

    mixed = jnp.concatenate([rows[0] * window, rows[1] * window], axis=1)
    swapped = jnp.concatenate(
        [side for j in range(2) for side in (-mixed[:, j * 128 + 64 : j * 128 + 128], mixed[:, j * 128 : j * 128 + 64])],
        axis=1,
    )
    mixed_high, mixed_low = halves(mixed)
    swapped_high, swapped_low = halves(swapped)
    real, imag = quarter_turn(facet_row, facet_col)
    for a in range(SIDE):
        here = slice(a * XM, (a + 1) * XM)
        grid = mm3(table_high[0, here], table_low[0, here], mixed_high, mixed_low)
        grid += mm3(table_high[1, here], table_low[1, here], swapped_high, swapped_low)
        block = jnp.transpose(grid)
        for b in range(SIDE):
            for j in range(2):
                at = j * 128 + b * PART
                re, im = block[at : at + PART], block[at + 64 : at + 64 + PART]
                pieces[a * SIDE + b, j * 32 : j * 32 + 16] = real * re - imag * im
                pieces[a * SIDE + b, j * 32 + 16 : j * 32 + 32] = real * im + imag * re
            pltpu.make_async_copy(pieces.at[a * SIDE + b], out.at[task_of[a * SIDE + b]], left.at[a * SIDE + b]).start()
    for n in range(NF):
        pltpu.make_async_copy(pieces.at[n], out.at[task_of[n]], left.at[n]).wait()


def misfit_kernel(contributions, *refs):
    *visible, out, sums = refs
    _, _, part = position()
    grids = contributions[0]
    for f in range(1, NF):
        grids = grids + contributions[f]
    counts = [jnp.max(visible[c][META + 1 : META + 2]) for c in range(CHANS)]
    row_of = [(iota((PART, XM), 0) + g * PART).astype(F32).astype(BF16) for g in range(XM // PART)]
    column_of = iota((2 * PART, XM), 0) & (PART - 1)
    one, zero = jnp.ones((PART, XM), BF16), jnp.zeros((PART, XM), BF16)

    def slots(c, first):
        seen, scale = visible[c], visible[c][META : META + 1]
        grid_high, grid_low = halves(grids[: 2 * PART] + scale * grids[2 * PART :])
        cells = seen[2 * ROWS + first : 2 * ROWS + first + GROUP].astype(jnp.int32)
        u, v = (cells >> 7).astype(F32), (cells & (XM - 1)) - part * PART
        hots, misses = [], []
        for r in range(GROUP):
            u_here = jnp.broadcast_to(u[r : r + 1], (PART, XM)).astype(BF16)
            hots.append(jnp.concatenate([jnp.where(rows == u_here, one, zero) for rows in row_of], axis=0))
        hot = jnp.concatenate(hots, axis=1)
        found = mm(jnp.concatenate([grid_high, grid_low], axis=0), hot)
        predicted = found[: 2 * PART] + found[2 * PART :]
        for r in range(GROUP):
            re = jnp.broadcast_to(seen[first + r : first + r + 1], (PART, XM))
            im = jnp.broadcast_to(seen[ROWS + first + r : ROWS + first + r + 1], (PART, XM))
            missed = jnp.concatenate([re, im], axis=0) - predicted[:, r * XM : (r + 1) * XM]
            misses.append(jnp.where(column_of == v[r : r + 1], missed, 0.0))
        missed = jnp.concatenate(halves(jnp.concatenate(misses, axis=1)), axis=0)
        return mm(hot, missed, ((1,), (1,))), scale[:, :PIECE]

    totals = [jnp.zeros((XM, PIECE), F32)] * 2
    for c in range(CHANS):
        made, scale = slots(c, 0)
        totals = [totals[0] + made, totals[1] + scale * made]
    sums[0], sums[1] = totals
    for first in range(GROUP, ROWS, GROUP):
        for c in range(CHANS):

            @pl.when(counts[c] > first * XM)
            def more(c=c, first=first):
                made, scale = slots(c, first)
                sums[0] += made
                sums[1] += scale * made

    turned = jnp.transpose(jnp.concatenate([sums[0], sums[1]], axis=1))
    result = jnp.concatenate([turned[0:32] + turned[32:64], turned[64:96] + turned[96:128]], axis=0)
    for f in range(NF):
        out[f] = result


def rows_kernel(assignment, pieces, table_high, table_low, *refs):
    *outs, placed, mixed = refs
    facet_row, facet_col, part = position()
    real, imag = quarter_turn(facet_row, facet_col)
    for t in range(NF):
        s = assignment[t]
        for j in range(2):
            re, im = pieces[t, j * 32 : j * 32 + 16], pieces[t, j * 32 + 16 : j * 32 + 32]
            placed[s, j * 32 : j * 32 + 16] = real * re + imag * im
            placed[s, j * 32 + 16 : j * 32 + 32] = real * im - imag * re
    blocks = {}
    for j in range(2):
        for c in range(2):
            at = j * 32 + c * 16
            blocks[j, c] = jnp.concatenate(
                [jnp.concatenate([placed[a * SIDE + b, at : at + 16] for a in range(SIDE)], axis=1) for b in range(SIDE)], axis=0
            )
    grid = jnp.concatenate([blocks[0, 0], blocks[0, 1], blocks[1, 0], blocks[1, 1]], axis=0)
    swapped = jnp.concatenate([blocks[0, 1], -blocks[0, 0], blocks[1, 1], -blocks[1, 0]], axis=0)
    grid_high, grid_low = halves(grid)
    swapped_high, swapped_low = halves(swapped)
    both = ((1,), (1,))
    mixed[...] = mm3(table_high[0], table_low[0], grid_high, grid_low, both) + mm3(
        table_high[1], table_low[1], swapped_high, swapped_low, both
    )
    for d in range(SIDE):
        for other in range(2):
            frm = ((part // 2 + d) % SIDE) * 128 + (part % 2 + other) % 2 * 64
            outs[d][other] = mixed[pl.ds(pl.multiple_of(frm, 64), 64)]


def columns_kernel(*refs):
    *mixed, table_high, table_low, out, perm_high, perm_low = refs
    _, _, part = position()
    for n in range(CHANS):
        d, other = n % SIDE, n // SIDE
        k = (part // 2 + SIDE - d) % SIDE * 2 + (part % 2 + other) % 2
        for b in range(SIDE):
            to = slice(n * 64 + b * PART, n * 64 + (b + 1) * PART)
            frm = pl.ds(pl.multiple_of(b * XM + k * PART, PART), PART)
            perm_high[:, to] = table_high[:, frm]
            perm_low[:, to] = table_low[:, frm]
    stripes = []
    for j in range(2):
        for c in range(2):
            at = j * 128 + c * 64
            stripes.append(jnp.concatenate([mixed[n][n // SIDE, :, at : at + 64] for n in range(CHANS)], axis=1))
    high, low = halves(jnp.concatenate(stripes, axis=0))
    real = mm3(high, low, perm_high[0], perm_low[0])
    imag = mm3(high, low, perm_high[1], perm_low[1])
    window = jnp.concatenate([taper(iota((64, XM), 0) + part * 64)] * (FS // XM), axis=1) * taper(iota((1, FS), 1))
    for j in range(2):
        re, im = slice(j * 128, j * 128 + 64), slice(j * 128 + 64, j * 128 + 128)
        out[j, 0] = window * (real[re] + imag[im])
        out[j, 1] = window * (real[im] - imag[re])


def call(kernel, shapes, in_specs, scratch=(), out_specs=None, **kwargs):
    return pl.pallas_call(
        kernel,
        out_shape=shapes,
        in_specs=in_specs,
        out_specs=out_specs or jax.tree.map(lambda _: VMEM, shapes),
        scratch_shapes=list(scratch),
        compiler_params=pltpu.CompilerParams(vmem_limit_bytes=LIMIT),
        **kwargs,
    )


def over_chan(sent):
    own = [sent[0]] + [lax.ppermute(sent[d], "chan", [(c, (c + 2 * d) % CHANS) for c in range(CHANS)]) for d in (1, 2, 3)]
    return own + [lax.ppermute(piece, "chan", [(c, c ^ 1) for c in range(CHANS)]) for piece in own]


def on_device(model_taylor, channel_offset, assignment, observed, uv_bins, vis_counts):
    table = jax.ShapeDtypeStruct((2, FS, FS), BF16)
    table_high, table_low, sent, message = call(
        forward_kernel,
        (table, table, jax.ShapeDtypeStruct((NF, PIECE, XM), F32), jax.ShapeDtypeStruct((MSG, XM), F32)),
        [HBM] * 6,
        [
            pltpu.VMEM((4, FS, FS), F32),
            pltpu.VMEM((2, VIS), F32),
            pltpu.VMEM((1, VIS), jnp.int32),
            pltpu.SMEM((1,), F32),
            pltpu.SMEM((1, 1), jnp.int32),
            pltpu.SMEM((NF,), jnp.int32),
            pltpu.SMEM((NF,), jnp.int32),
            pltpu.VMEM((2, FS, 128), BF16),
            pltpu.VMEM((2, FS, 128), BF16),
            pltpu.VMEM((2, FS, 128), F32),
            pltpu.VMEM((NF, PIECE, XM), F32),
            pltpu.SemaphoreType.DMA((9,)),
            pltpu.SemaphoreType.DMA((NF,)),
        ],
        (VMEM, VMEM, HBM, VMEM),
    )(channel_offset, vis_counts, *(pltpu.with_memory_space_constraint(x, pltpu.HBM) for x in (assignment, model_taylor[:, 0], observed[0, 0], uv_bins[0])))
    received = lax.all_to_all(sent, "facet", 0, 0, tiled=True)
    visible = over_chan([message] * SIDE)
    copies = call(
        misfit_kernel,
        jax.ShapeDtypeStruct((NF, PIECE, XM), F32),
        [VMEM] * (1 + CHANS),
        [pltpu.VMEM((2, XM, PIECE), F32)],
    )(received, *visible)
    gathered = lax.all_to_all(copies, "facet", 0, 0, tiled=True)

    mixed = call(
        rows_kernel,
        (jax.ShapeDtypeStruct((2, 64, 256), F32),) * SIDE,
        [SMEM, VMEM, VMEM, VMEM],
        [pltpu.VMEM((NF, PIECE, XM), F32), pltpu.VMEM((FS, 256), F32)],
    )(assignment, gathered, table_high, table_low)
    stripes = over_chan(mixed)

    planes = call(
        columns_kernel,
        jax.ShapeDtypeStruct((2, 2, 64, FS), F32),
        [VMEM] * (CHANS + 2),
        [pltpu.VMEM((2, FS, FS), BF16), pltpu.VMEM((2, FS, FS), BF16)],
    )(*stripes, table_high, table_low)
    return planes[:, None]


def solution(mesh):
    return jax.shard_map(
        on_device,
        mesh=mesh,
        in_specs=(
            P(None, "facet", None, None, None),
            P("chan"),
            P(),
            P("chan", "facet", None, None),
            P("chan", "facet", None),
            P("chan", "facet"),
        ),
        out_specs=P(None, "facet", None, "chan", None),
        check_vma=False,
    )
```

```python
import jax
import jax.numpy as jnp
from jax import lax
from jax.experimental import pallas as pl
from jax.experimental.pallas import tpu as pltpu
from jax.sharding import PartitionSpec as P


FS = 512
XM = 128
SIDE = 4
NF = 16
CHANS = 8
VIS = 4096
IMAGE = 2048
PART = XM // CHANS
PIECE = 4 * PART
ROWS = VIS // XM
META = 3 * ROWS
MSG = META + 8
GROUP = 16

LIMIT = 24 << 20
TURN = 6.283185307179586 / IMAGE
F32 = jnp.float32
BF16 = jnp.bfloat16
VMEM = pl.BlockSpec(memory_space=pltpu.VMEM)
SMEM = pl.BlockSpec(memory_space=pltpu.SMEM)
HBM = pl.BlockSpec(memory_space=pltpu.HBM)


def cos_turn(m):
    m = m & (IMAGE - 1)
    quarter = (m + 256) >> 9
    t = (m - (quarter << 9)).astype(F32) * TURN
    t2 = t * t
    even = 1.0 + t2 * (-0.5 + t2 * (1 / 24 + t2 * (-1 / 720 + t2 * (1 / 40320 - t2 * (1 / 3628800)))))
    odd = t * (1.0 + t2 * (-1 / 6 + t2 * (1 / 120 + t2 * (-1 / 5040 + t2 * (1 / 362880)))))
    value = jnp.where((quarter & 1) == 1, odd, even)
    return jnp.where(((quarter + 1) & 2) == 2, -value, value)


def taper(n):
    return (0.55 + 0.45 * cos_turn(4 * n - (2 * FS - 2))) * F32(1.0 / FS**0.5)


def halves(value):
    high = value.astype(BF16)
    return high, (value - high.astype(F32)).astype(BF16)


def iota(shape, dim):
    return lax.broadcasted_iota(jnp.int32, shape, dim)


def mm(a, b, dims=((1,), (0,))):
    return lax.dot_general(a, b, (dims, ((), ())), preferred_element_type=F32)


def mm3(a_high, a_low, b_high, b_low, dims=((1,), (0,))):
    return mm(a_high, b_high, dims) + (mm(a_high, b_low, dims) + mm(a_low, b_high, dims))


def position():
    facet = lax.axis_index("facet")
    return facet // SIDE, facet % SIDE, lax.axis_index("chan")


def quarter_turn(facet_row, facet_col):
    shape = (PART, XM)
    turn = (iota(shape, 1) * facet_row + iota(shape, 0) * facet_col) & 3
    real = jnp.where(turn == 0, 1.0, jnp.where(turn == 2, -1.0, 0.0)).astype(F32)
    imag = jnp.where(turn == 3, 1.0, jnp.where(turn == 1, -1.0, 0.0)).astype(F32)
    return real, imag


def forward_kernel(
    offset, count, assignment, sky, observed, bins, table_high, table_low, out, message,
    image, seen, cells, offset_here, count_here, order, task_of, cols_high, cols_low, rows, pieces, arrived, left,
):
    facet_row, facet_col, part = position()
    small = [
        pltpu.make_async_copy(frm, to, arrived.at[n])
        for n, (frm, to) in enumerate(
            ((offset, offset_here), (count, count_here), (assignment, order), (observed, seen), (bins, cells))
        )
    ]
    planes = [pltpu.make_async_copy(sky.at[n // 2, n % 2], image.at[n], arrived.at[5 + n]) for n in range(4)]
    for copy in planes + small:
        copy.start()

    lane = iota((PART, XM), 1)
    column = ((lane & 63) >> 4) * XM + part * PART + (lane & (PART - 1))
    side = jnp.where(lane >= 64, 512, 0)
    fine_y = column * iota((PART, XM), 0) + side
    fine_one, fine_two = cos_turn(fine_y), cos_turn(fine_y + 512)
    lane = iota((FS // PART, XM), 1)
    column = ((lane & 63) >> 4) * XM + part * PART + (lane & (PART - 1))
    coarse_y = column * PART * iota((FS // PART, XM), 0)
    coarse_re, coarse_im = cos_turn(coarse_y), cos_turn(coarse_y + 512)
    window = jnp.transpose(jnp.broadcast_to(taper(iota((1, FS), 1)), (XM, FS)))
    for g in range(FS // PART):
        here = slice(g * PART, (g + 1) * PART)
        re, im = coarse_re[g : g + 1] * window[here], coarse_im[g : g + 1] * window[here]
        cols_high[0, here], cols_low[0, here] = halves(re * fine_one - im * fine_two)
        cols_high[1, here], cols_low[1, here] = halves(-(im * fine_one + re * fine_two))

    fine = iota((PART, FS), 0) * iota((PART, FS), 1)
    fine_re, fine_im = cos_turn(fine), cos_turn(fine + 512)
    coarse = iota((FS // PART, FS), 0) * PART * iota((FS // PART, FS), 1)
    coarse_re, coarse_im = cos_turn(coarse), cos_turn(coarse + 512)

    for g in range(FS // PART):
        re, im = coarse_re[g : g + 1], coarse_im[g : g + 1]
        here = slice(g * PART, (g + 1) * PART)
        table_high[0, here], table_low[0, here] = halves(re * fine_re - im * fine_im)
        table_high[1, here], table_low[1, here] = halves(re * fine_im + im * fine_re)

    for n in range(4):
        planes[n].wait()
        high, low = halves(image[n])
        both = mm(high, jnp.concatenate([cols_high[n % 2], cols_low[n % 2]], axis=1))
        made = both[:, :128] + (both[:, 128:] + mm(low, cols_high[n % 2]))
        if n % 2 == 0:
            rows[n // 2] = made
        else:
            rows[n // 2] += made

    for copy in small:
        copy.wait()
    for t in range(NF):
        task_of[order[t]] = t
    live = iota((1, VIS), 1) < count_here[0, 0]
    marked = jnp.where(live, cells[...].astype(F32), -1.0)
    for row in range(ROWS):
        lanes = slice(row * XM, (row + 1) * XM)
        message[row : row + 1, :] = seen[0:1, lanes]
        message[ROWS + row : ROWS + row + 1, :] = seen[1:2, lanes]
        message[2 * ROWS + row : 2 * ROWS + row + 1, :] = marked[:, lanes]
    place = iota((8, XM), 0)
    meta = jnp.where(place == 0, offset_here[0], jnp.where(place == 1, count_here[0, 0].astype(F32), 0.0))
    message[META:MSG, :] = meta

    mixed = jnp.concatenate([rows[0] * window, rows[1] * window], axis=1)
    swapped = jnp.concatenate(
        [side for j in range(2) for side in (-mixed[:, j * 128 + 64 : j * 128 + 128], mixed[:, j * 128 : j * 128 + 64])],
        axis=1,
    )
    mixed_high, mixed_low = halves(mixed)
    swapped_high, swapped_low = halves(swapped)
    real, imag = quarter_turn(facet_row, facet_col)
    for a in range(SIDE):
        here = slice(a * XM, (a + 1) * XM)
        grid = mm3(table_high[0, here], table_low[0, here], mixed_high, mixed_low)
        grid += mm3(table_high[1, here], table_low[1, here], swapped_high, swapped_low)
        block = jnp.transpose(grid)
        for b in range(SIDE):
            for j in range(2):
                at = j * 128 + b * PART
                re, im = block[at : at + PART], block[at + 64 : at + 64 + PART]
                pieces[a * SIDE + b, j * 32 : j * 32 + 16] = real * re - imag * im
                pieces[a * SIDE + b, j * 32 + 16 : j * 32 + 32] = real * im + imag * re
            pltpu.make_async_copy(pieces.at[a * SIDE + b], out.at[task_of[a * SIDE + b]], left.at[a * SIDE + b]).start()
    for n in range(NF):
        pltpu.make_async_copy(pieces.at[n], out.at[task_of[n]], left.at[n]).wait()


def misfit_kernel(contributions, *refs):
    *visible, out, sums = refs
    _, _, part = position()
    grids = contributions[0]
    for f in range(1, NF):
        grids = grids + contributions[f]
    counts = [jnp.max(visible[c][META + 1 : META + 2]) for c in range(CHANS)]
    row_of = [(iota((PART, XM), 0) + g * PART).astype(F32).astype(BF16) for g in range(XM // PART)]
    column_of = iota((2 * PART, XM), 0) & (PART - 1)
    one, zero = jnp.ones((PART, XM), BF16), jnp.zeros((PART, XM), BF16)

    def slots(c, first):
        seen, scale = visible[c], visible[c][META : META + 1]
        grid_high, grid_low = halves(grids[: 2 * PART] + scale * grids[2 * PART :])
        cells = seen[2 * ROWS + first : 2 * ROWS + first + GROUP].astype(jnp.int32)
        u, v = (cells >> 7).astype(F32), (cells & (XM - 1)) - part * PART
        hots, misses = [], []
        for r in range(GROUP):
            u_here = jnp.broadcast_to(u[r : r + 1], (PART, XM)).astype(BF16)
            hots.append(jnp.concatenate([jnp.where(rows == u_here, one, zero) for rows in row_of], axis=0))
        hot = jnp.concatenate(hots, axis=1)
        found = mm(jnp.concatenate([grid_high, grid_low], axis=0), hot)
        predicted = found[: 2 * PART] + found[2 * PART :]
        for r in range(GROUP):
            re = jnp.broadcast_to(seen[first + r : first + r + 1], (PART, XM))
            im = jnp.broadcast_to(seen[ROWS + first + r : ROWS + first + r + 1], (PART, XM))
            missed = jnp.concatenate([re, im], axis=0) - predicted[:, r * XM : (r + 1) * XM]
            misses.append(jnp.where(column_of == v[r : r + 1], missed, 0.0))
        missed = jnp.concatenate(halves(jnp.concatenate(misses, axis=1)), axis=0)
        return mm(hot, missed, ((1,), (1,))), scale[:, :PIECE]

    totals = [jnp.zeros((XM, PIECE), F32)] * 2
    for c in range(CHANS):
        made, scale = slots(c, 0)
        totals = [totals[0] + made, totals[1] + scale * made]
    sums[0], sums[1] = totals
    for first in range(GROUP, ROWS, GROUP):
        for c in range(CHANS):

            @pl.when(counts[c] > first * XM)
            def more(c=c, first=first):
                made, scale = slots(c, first)
                sums[0] += made
                sums[1] += scale * made

    turned = jnp.transpose(jnp.concatenate([sums[0], sums[1]], axis=1))
    result = jnp.concatenate([turned[0:32] + turned[32:64], turned[64:96] + turned[96:128]], axis=0)
    for f in range(NF):
        out[f] = result


def rows_kernel(assignment, pieces, table_high, table_low, *refs):
    *outs, placed, mixed = refs
    facet_row, facet_col, part = position()
    real, imag = quarter_turn(facet_row, facet_col)
    for t in range(NF):
        s = assignment[t]
        for j in range(2):
            re, im = pieces[t, j * 32 : j * 32 + 16], pieces[t, j * 32 + 16 : j * 32 + 32]
            placed[s, j * 32 : j * 32 + 16] = real * re + imag * im
            placed[s, j * 32 + 16 : j * 32 + 32] = real * im - imag * re
    blocks = {}
    for j in range(2):
        for c in range(2):
            at = j * 32 + c * 16
            blocks[j, c] = jnp.concatenate(
                [jnp.concatenate([placed[a * SIDE + b, at : at + 16] for a in range(SIDE)], axis=1) for b in range(SIDE)], axis=0
            )
    grid = jnp.concatenate([blocks[0, 0], blocks[0, 1], blocks[1, 0], blocks[1, 1]], axis=0)
    swapped = jnp.concatenate([blocks[0, 1], -blocks[0, 0], blocks[1, 1], -blocks[1, 0]], axis=0)
    grid_high, grid_low = halves(grid)
    swapped_high, swapped_low = halves(swapped)
    both = ((1,), (1,))
    mixed[...] = mm3(table_high[0], table_low[0], grid_high, grid_low, both) + mm3(
        table_high[1], table_low[1], swapped_high, swapped_low, both
    )
    for d in range(SIDE):
        for other in range(2):
            frm = ((part // 2 + d) % SIDE) * 128 + (part % 2 + other) % 2 * 64
            outs[d][other] = mixed[pl.ds(pl.multiple_of(frm, 64), 64)]


def columns_kernel(*refs):
    *mixed, table_high, table_low, out, perm_high, perm_low = refs
    _, _, part = position()
    for n in range(CHANS):
        d, other = n % SIDE, n // SIDE
        k = (part // 2 + SIDE - d) % SIDE * 2 + (part % 2 + other) % 2
        for b in range(SIDE):
            to = slice(n * 64 + b * PART, n * 64 + (b + 1) * PART)
            frm = pl.ds(pl.multiple_of(b * XM + k * PART, PART), PART)
            perm_high[:, to] = table_high[:, frm]
            perm_low[:, to] = table_low[:, frm]
    stripes = []
    for j in range(2):
        for c in range(2):
            at = j * 128 + c * 64
            stripes.append(jnp.concatenate([mixed[n][n // SIDE, :, at : at + 64] for n in range(CHANS)], axis=1))
    high, low = halves(jnp.concatenate(stripes, axis=0))
    real = mm3(high, low, perm_high[0], perm_low[0])
    imag = mm3(high, low, perm_high[1], perm_low[1])
    window = jnp.concatenate([taper(iota((64, XM), 0) + part * 64)] * (FS // XM), axis=1) * taper(iota((1, FS), 1))
    for j in range(2):
        re, im = slice(j * 128, j * 128 + 64), slice(j * 128 + 64, j * 128 + 128)
        out[j, 0] = window * (real[re] + imag[im])
        out[j, 1] = window * (real[im] - imag[re])


def call(kernel, shapes, in_specs, scratch=(), out_specs=None, **kwargs):
    return pl.pallas_call(
        kernel,
        out_shape=shapes,
        in_specs=in_specs,
        out_specs=out_specs or jax.tree.map(lambda _: VMEM, shapes),
        scratch_shapes=list(scratch),
        compiler_params=pltpu.CompilerParams(vmem_limit_bytes=LIMIT),
        **kwargs,
    )


def over_chan(sent, order=(1, 2, 3)):
    own = [sent[0]] + [lax.ppermute(sent[d], "chan", [(c, (c + 2 * d) % CHANS) for c in range(CHANS)]) for d in order]
    return own + [lax.ppermute(piece, "chan", [(c, c ^ 1) for c in range(CHANS)]) for piece in own]


def on_device(model_taylor, channel_offset, assignment, observed, uv_bins, vis_counts):
    table = jax.ShapeDtypeStruct((2, FS, FS), BF16)
    table_high, table_low, sent, message = call(
        forward_kernel,
        (table, table, jax.ShapeDtypeStruct((NF, PIECE, XM), F32), jax.ShapeDtypeStruct((MSG, XM), F32)),
        [HBM] * 6,
        [
            pltpu.VMEM((4, FS, FS), F32),
            pltpu.VMEM((2, VIS), F32),
            pltpu.VMEM((1, VIS), jnp.int32),
            pltpu.SMEM((1,), F32),
            pltpu.SMEM((1, 1), jnp.int32),
            pltpu.SMEM((NF,), jnp.int32),
            pltpu.SMEM((NF,), jnp.int32),
            pltpu.VMEM((2, FS, 128), BF16),
            pltpu.VMEM((2, FS, 128), BF16),
            pltpu.VMEM((2, FS, 128), F32),
            pltpu.VMEM((NF, PIECE, XM), F32),
            pltpu.SemaphoreType.DMA((9,)),
            pltpu.SemaphoreType.DMA((NF,)),
        ],
        (VMEM, VMEM, HBM, VMEM),
    )(channel_offset, vis_counts, *(pltpu.with_memory_space_constraint(x, pltpu.HBM) for x in (assignment, model_taylor[:, 0], observed[0, 0], uv_bins[0])))
    received = lax.all_to_all(sent, "facet", 0, 0, tiled=True)
    visible = over_chan([message] * SIDE, (2, 3, 1))
    copies = call(
        misfit_kernel,
        jax.ShapeDtypeStruct((NF, PIECE, XM), F32),
        [VMEM] * (1 + CHANS),
        [pltpu.VMEM((2, XM, PIECE), F32)],
    )(received, *visible)
    gathered = lax.all_to_all(copies, "facet", 0, 0, tiled=True)

    mixed = call(
        rows_kernel,
        (jax.ShapeDtypeStruct((2, 64, 256), F32),) * SIDE,
        [SMEM, VMEM, VMEM, VMEM],
        [pltpu.VMEM((NF, PIECE, XM), F32), pltpu.VMEM((FS, 256), F32)],
    )(assignment, gathered, table_high, table_low)
    stripes = over_chan(mixed)

    planes = call(
        columns_kernel,
        jax.ShapeDtypeStruct((2, 2, 64, FS), F32),
        [VMEM] * (CHANS + 2),
        [pltpu.VMEM((2, FS, FS), BF16), pltpu.VMEM((2, FS, FS), BF16)],
    )(*stripes, table_high, table_low)
    return planes[:, None]


def solution(mesh):
    return jax.shard_map(
        on_device,
        mesh=mesh,
        in_specs=(
            P(None, "facet", None, None, None),
            P("chan"),
            P(),
            P("chan", "facet", None, None),
            P("chan", "facet", None),
            P("chan", "facet"),
        ),
        out_specs=P(None, "facet", None, "chan", None),
        check_vma=False,
    )
```

```python
import jax
import jax.numpy as jnp
from jax import lax
from jax.experimental import pallas as pl
from jax.experimental.pallas import tpu as pltpu
from jax.sharding import PartitionSpec as P


FS = 512
XM = 128
SIDE = 4
NF = 16
CHANS = 8
VIS = 4096
IMAGE = 2048
PART = XM // CHANS
PIECE = 4 * PART
ROWS = VIS // XM
META = 3 * ROWS
MSG = META + 8
GROUP = 16

LIMIT = 24 << 20
TURN = 6.283185307179586 / IMAGE
F32 = jnp.float32
BF16 = jnp.bfloat16
VMEM = pl.BlockSpec(memory_space=pltpu.VMEM)
SMEM = pl.BlockSpec(memory_space=pltpu.SMEM)
HBM = pl.BlockSpec(memory_space=pltpu.HBM)


def cos_turn(m):
    m = m & (IMAGE - 1)
    quarter = (m + 256) >> 9
    t = (m - (quarter << 9)).astype(F32) * TURN
    t2 = t * t
    even = 1.0 + t2 * (-0.5 + t2 * (1 / 24 + t2 * (-1 / 720 + t2 * (1 / 40320 - t2 * (1 / 3628800)))))
    odd = t * (1.0 + t2 * (-1 / 6 + t2 * (1 / 120 + t2 * (-1 / 5040 + t2 * (1 / 362880)))))
    value = jnp.where((quarter & 1) == 1, odd, even)
    return jnp.where(((quarter + 1) & 2) == 2, -value, value)


def taper(n):
    return (0.55 + 0.45 * cos_turn(4 * n - (2 * FS - 2))) * F32(1.0 / FS**0.5)


def halves(value):
    high = value.astype(BF16)
    return high, (value - high.astype(F32)).astype(BF16)


def iota(shape, dim):
    return lax.broadcasted_iota(jnp.int32, shape, dim)


def mm(a, b, dims=((1,), (0,))):
    return lax.dot_general(a, b, (dims, ((), ())), preferred_element_type=F32)


def mm3(a_high, a_low, b_high, b_low, dims=((1,), (0,))):
    return mm(a_high, b_high, dims) + (mm(a_high, b_low, dims) + mm(a_low, b_high, dims))


def position():
    facet = lax.axis_index("facet")
    return facet // SIDE, facet % SIDE, lax.axis_index("chan")


def quarter_turn(facet_row, facet_col):
    shape = (PART, XM)
    turn = (iota(shape, 1) * facet_row + iota(shape, 0) * facet_col) & 3
    real = jnp.where(turn == 0, 1.0, jnp.where(turn == 2, -1.0, 0.0)).astype(F32)
    imag = jnp.where(turn == 3, 1.0, jnp.where(turn == 1, -1.0, 0.0)).astype(F32)
    return real, imag


def forward_kernel(
    offset, count, assignment, sky, observed, bins, table_high, table_low, out, message,
    image, seen, cells, offset_here, count_here, order, task_of, cols_high, cols_low, rows, pieces, arrived, left,
):
    facet_row, facet_col, part = position()
    small = [
        pltpu.make_async_copy(frm, to, arrived.at[n])
        for n, (frm, to) in enumerate(
            ((offset, offset_here), (count, count_here), (assignment, order), (observed, seen), (bins, cells))
        )
    ]
    planes = [pltpu.make_async_copy(sky.at[n // 2, n % 2], image.at[n], arrived.at[5 + n]) for n in range(4)]
    for copy in planes + small:
        copy.start()

    lane = iota((PART, XM), 1)
    column = ((lane & 63) >> 4) * XM + part * PART + (lane & (PART - 1))
    side = jnp.where(lane >= 64, 512, 0)
    fine_y = column * iota((PART, XM), 0) + side
    fine_one, fine_two = cos_turn(fine_y), cos_turn(fine_y + 512)
    lane = iota((FS // PART, XM), 1)
    column = ((lane & 63) >> 4) * XM + part * PART + (lane & (PART - 1))
    coarse_y = column * PART * iota((FS // PART, XM), 0)
    coarse_re, coarse_im = cos_turn(coarse_y), cos_turn(coarse_y + 512)
    window = jnp.transpose(jnp.broadcast_to(taper(iota((1, FS), 1)), (XM, FS)))
    for g in range(FS // PART):
        here = slice(g * PART, (g + 1) * PART)
        re, im = coarse_re[g : g + 1] * window[here], coarse_im[g : g + 1] * window[here]
        cols_high[0, here], cols_low[0, here] = halves(re * fine_one - im * fine_two)
        cols_high[1, here], cols_low[1, here] = halves(-(im * fine_one + re * fine_two))

    fine = iota((PART, FS), 0) * iota((PART, FS), 1)
    fine_re, fine_im = cos_turn(fine), cos_turn(fine + 512)
    coarse = iota((FS // PART, FS), 0) * PART * iota((FS // PART, FS), 1)
    coarse_re, coarse_im = cos_turn(coarse), cos_turn(coarse + 512)

    for g in range(FS // PART):
        re, im = coarse_re[g : g + 1], coarse_im[g : g + 1]
        here = slice(g * PART, (g + 1) * PART)
        table_high[0, here], table_low[0, here] = halves(re * fine_re - im * fine_im)
        table_high[1, here], table_low[1, here] = halves(re * fine_im + im * fine_re)

    for n in range(4):
        planes[n].wait()
        high, low = halves(image[n])
        both = mm(high, jnp.concatenate([cols_high[n % 2], cols_low[n % 2]], axis=1))
        made = both[:, :128] + (both[:, 128:] + mm(low, cols_high[n % 2]))
        if n % 2 == 0:
            rows[n // 2] = made
        else:
            rows[n // 2] += made

    for copy in small:
        copy.wait()
    for t in range(NF):
        task_of[order[t]] = t
    live = iota((1, VIS), 1) < count_here[0, 0]
    marked = jnp.where(live, cells[...].astype(F32), -1.0)
    for row in range(ROWS):
        lanes = slice(row * XM, (row + 1) * XM)
        message[row : row + 1, :] = seen[0:1, lanes]
        message[ROWS + row : ROWS + row + 1, :] = seen[1:2, lanes]
        message[2 * ROWS + row : 2 * ROWS + row + 1, :] = marked[:, lanes]
    place = iota((8, XM), 0)
    meta = jnp.where(place == 0, offset_here[0], jnp.where(place == 1, count_here[0, 0].astype(F32), 0.0))
    message[META:MSG, :] = meta

    mixed = jnp.concatenate([rows[0] * window, rows[1] * window], axis=1)
    swapped = jnp.concatenate(
        [side for j in range(2) for side in (-mixed[:, j * 128 + 64 : j * 128 + 128], mixed[:, j * 128 : j * 128 + 64])],
        axis=1,
    )
    mixed_high, mixed_low = halves(mixed)
    swapped_high, swapped_low = halves(swapped)
    real, imag = quarter_turn(facet_row, facet_col)
    for a in range(SIDE):
        here = slice(a * XM, (a + 1) * XM)
        grid = mm3(table_high[0, here], table_low[0, here], mixed_high, mixed_low)
        grid += mm3(table_high[1, here], table_low[1, here], swapped_high, swapped_low)
        block = jnp.transpose(grid)
        for b in range(SIDE):
            for j in range(2):
                at = j * 128 + b * PART
                re, im = block[at : at + PART], block[at + 64 : at + 64 + PART]
                pieces[a * SIDE + b, j * 32 : j * 32 + 16] = real * re - imag * im
                pieces[a * SIDE + b, j * 32 + 16 : j * 32 + 32] = real * im + imag * re
            pltpu.make_async_copy(pieces.at[a * SIDE + b], out.at[task_of[a * SIDE + b]], left.at[a * SIDE + b]).start()
    for n in range(NF):
        pltpu.make_async_copy(pieces.at[n], out.at[task_of[n]], left.at[n]).wait()


def misfit_kernel(contributions, *refs):
    *visible, out, sums = refs
    _, _, part = position()
    grids = contributions[0]
    for f in range(1, NF):
        grids = grids + contributions[f]
    counts = [jnp.max(visible[c][META + 1 : META + 2]) for c in range(CHANS)]
    row_of = [(iota((PART, XM), 0) + g * PART).astype(F32).astype(BF16) for g in range(XM // PART)]
    column_of = iota((2 * PART, XM), 0) & (PART - 1)
    one, zero = jnp.ones((PART, XM), BF16), jnp.zeros((PART, XM), BF16)

    def slots(c, first):
        seen, scale = visible[c], visible[c][META : META + 1]
        grid_high, grid_low = halves(grids[: 2 * PART] + scale * grids[2 * PART :])
        cells = seen[2 * ROWS + first : 2 * ROWS + first + GROUP].astype(jnp.int32)
        u, v = (cells >> 7).astype(F32), (cells & (XM - 1)) - part * PART
        hots, misses = [], []
        for r in range(GROUP):
            u_here = jnp.broadcast_to(u[r : r + 1], (PART, XM)).astype(BF16)
            hots.append(jnp.concatenate([jnp.where(rows == u_here, one, zero) for rows in row_of], axis=0))
        hot = jnp.concatenate(hots, axis=1)
        found = mm(jnp.concatenate([grid_high, grid_low], axis=0), hot)
        predicted = found[: 2 * PART] + found[2 * PART :]
        for r in range(GROUP):
            re = jnp.broadcast_to(seen[first + r : first + r + 1], (PART, XM))
            im = jnp.broadcast_to(seen[ROWS + first + r : ROWS + first + r + 1], (PART, XM))
            missed = jnp.concatenate([re, im], axis=0) - predicted[:, r * XM : (r + 1) * XM]
            misses.append(jnp.where(column_of == v[r : r + 1], missed, 0.0))
        missed = jnp.concatenate(halves(jnp.concatenate(misses, axis=1)), axis=0)
        return mm(hot, missed, ((1,), (1,))), scale[:, :PIECE]

    totals = [jnp.zeros((XM, PIECE), F32)] * 2
    for c in range(CHANS):
        made, scale = slots(c, 0)
        totals = [totals[0] + made, totals[1] + scale * made]
    sums[0], sums[1] = totals
    for first in range(GROUP, ROWS, GROUP):
        for c in range(CHANS):

            @pl.when(counts[c] > first * XM)
            def more(c=c, first=first):
                made, scale = slots(c, first)
                sums[0] += made
                sums[1] += scale * made

    turned = jnp.transpose(jnp.concatenate([sums[0], sums[1]], axis=1))
    result = jnp.concatenate([turned[0:32] + turned[32:64], turned[64:96] + turned[96:128]], axis=0)
    for f in range(NF):
        out[f] = result


def rows_kernel(assignment, pieces, table_high, table_low, *refs):
    *outs, placed, mixed = refs
    facet_row, facet_col, part = position()
    real, imag = quarter_turn(facet_row, facet_col)
    for t in range(NF):
        s = assignment[t]
        for j in range(2):
            re, im = pieces[t, j * 32 : j * 32 + 16], pieces[t, j * 32 + 16 : j * 32 + 32]
            placed[s, j * 32 : j * 32 + 16] = real * re + imag * im
            placed[s, j * 32 + 16 : j * 32 + 32] = real * im - imag * re
    blocks = {}
    for j in range(2):
        for c in range(2):
            at = j * 32 + c * 16
            blocks[j, c] = jnp.concatenate(
                [jnp.concatenate([placed[a * SIDE + b, at : at + 16] for a in range(SIDE)], axis=1) for b in range(SIDE)], axis=0
            )
    grid = jnp.concatenate([blocks[0, 0], blocks[0, 1], blocks[1, 0], blocks[1, 1]], axis=0)
    swapped = jnp.concatenate([blocks[0, 1], -blocks[0, 0], blocks[1, 1], -blocks[1, 0]], axis=0)
    grid_high, grid_low = halves(grid)
    swapped_high, swapped_low = halves(swapped)
    both = ((1,), (1,))
    mixed[...] = mm3(table_high[0], table_low[0], grid_high, grid_low, both) + mm3(
        table_high[1], table_low[1], swapped_high, swapped_low, both
    )
    for d in range(SIDE):
        for other in range(2):
            frm = ((part // 2 + d) % SIDE) * 128 + (part % 2 + other) % 2 * 64
            outs[d][other] = mixed[pl.ds(pl.multiple_of(frm, 64), 64)]


def order_kernel(table_high, table_low, perm_high, perm_low):
    _, _, part = position()
    for n in range(CHANS):
        d, other = n % SIDE, n // SIDE
        k = (part // 2 + SIDE - d) % SIDE * 2 + (part % 2 + other) % 2
        for b in range(SIDE):
            to = slice(n * 64 + b * PART, n * 64 + (b + 1) * PART)
            frm = pl.ds(pl.multiple_of(b * XM + k * PART, PART), PART)
            perm_high[:, to] = table_high[:, frm]
            perm_low[:, to] = table_low[:, frm]


def columns_kernel(*refs):
    *mixed, perm_high, perm_low, out = refs
    _, _, part = position()
    stripes = []
    for j in range(2):
        for c in range(2):
            at = j * 128 + c * 64
            stripes.append(jnp.concatenate([mixed[n][n // SIDE, :, at : at + 64] for n in range(CHANS)], axis=1))
    high, low = halves(jnp.concatenate(stripes, axis=0))
    real = mm3(high, low, perm_high[0], perm_low[0])
    imag = mm3(high, low, perm_high[1], perm_low[1])
    window = jnp.concatenate([taper(iota((64, XM), 0) + part * 64)] * (FS // XM), axis=1) * taper(iota((1, FS), 1))
    for j in range(2):
        re, im = slice(j * 128, j * 128 + 64), slice(j * 128 + 64, j * 128 + 128)
        out[j, 0] = window * (real[re] + imag[im])
        out[j, 1] = window * (real[im] - imag[re])


def call(kernel, shapes, in_specs, scratch=(), out_specs=None, **kwargs):
    return pl.pallas_call(
        kernel,
        out_shape=shapes,
        in_specs=in_specs,
        out_specs=out_specs or jax.tree.map(lambda _: VMEM, shapes),
        scratch_shapes=list(scratch),
        compiler_params=pltpu.CompilerParams(vmem_limit_bytes=LIMIT),
        **kwargs,
    )


def over_chan(sent, order=(1, 2, 3)):
    own = [sent[0]] + [lax.ppermute(sent[d], "chan", [(c, (c + 2 * d) % CHANS) for c in range(CHANS)]) for d in order]
    return own + [lax.ppermute(piece, "chan", [(c, c ^ 1) for c in range(CHANS)]) for piece in own]


def on_device(model_taylor, channel_offset, assignment, observed, uv_bins, vis_counts):
    table = jax.ShapeDtypeStruct((2, FS, FS), BF16)
    table_high, table_low, sent, message = call(
        forward_kernel,
        (table, table, jax.ShapeDtypeStruct((NF, PIECE, XM), F32), jax.ShapeDtypeStruct((MSG, XM), F32)),
        [HBM] * 6,
        [
            pltpu.VMEM((4, FS, FS), F32),
            pltpu.VMEM((2, VIS), F32),
            pltpu.VMEM((1, VIS), jnp.int32),
            pltpu.SMEM((1,), F32),
            pltpu.SMEM((1, 1), jnp.int32),
            pltpu.SMEM((NF,), jnp.int32),
            pltpu.SMEM((NF,), jnp.int32),
            pltpu.VMEM((2, FS, 128), BF16),
            pltpu.VMEM((2, FS, 128), BF16),
            pltpu.VMEM((2, FS, 128), F32),
            pltpu.VMEM((NF, PIECE, XM), F32),
            pltpu.SemaphoreType.DMA((9,)),
            pltpu.SemaphoreType.DMA((NF,)),
        ],
        (VMEM, VMEM, HBM, VMEM),
    )(channel_offset, vis_counts, *(pltpu.with_memory_space_constraint(x, pltpu.HBM) for x in (assignment, model_taylor[:, 0], observed[0, 0], uv_bins[0])))
    received = lax.all_to_all(sent, "facet", 0, 0, tiled=True)
    visible = over_chan([message] * SIDE, (2, 3, 1))
    copies = call(
        misfit_kernel,
        jax.ShapeDtypeStruct((NF, PIECE, XM), F32),
        [VMEM] * (1 + CHANS),
        [pltpu.VMEM((2, XM, PIECE), F32)],
    )(received, *visible)
    gathered = lax.all_to_all(copies, "facet", 0, 0, tiled=True)

    mixed = call(
        rows_kernel,
        (jax.ShapeDtypeStruct((2, 64, 256), F32),) * SIDE,
        [SMEM, VMEM, VMEM, VMEM],
        [pltpu.VMEM((NF, PIECE, XM), F32), pltpu.VMEM((FS, 256), F32)],
    )(assignment, gathered, table_high, table_low)
    stripes = over_chan(mixed)
    perm_high, perm_low = call(order_kernel, (table, table), [VMEM, VMEM])(table_high, table_low)

    planes = call(
        columns_kernel,
        jax.ShapeDtypeStruct((2, 2, 64, FS), F32),
        [VMEM] * (CHANS + 2),
    )(*stripes, perm_high, perm_low)
    return planes[:, None]


def solution(mesh):
    return jax.shard_map(
        on_device,
        mesh=mesh,
        in_specs=(
            P(None, "facet", None, None, None),
            P("chan"),
            P(),
            P("chan", "facet", None, None),
            P("chan", "facet", None),
            P("chan", "facet"),
        ),
        out_specs=P(None, "facet", None, "chan", None),
        check_vma=False,
    )
```
